256 devices in a mesh: row: 16 (over y, z_lo, core), col: 16 (over z_hi, x).
Axes of the slice: x: 4, y: 4, z: 8 (z_hi: 4, z_lo: 2; z = z_hi * 2 + z_lo), core: 2. Of those that a mesh axis runs over, the one named last changes fastest.
Arguments:
- upper_corner: bfloat16 [96, 96], P(None, 'row'), may hold values from -6 to 6
- right_corner: bfloat16 [96, 96], P(None, 'row'), may hold values from -6 to 6
- lower_corner: bfloat16 [96, 96], P(None, 'row'), may hold values from -6 to 6
- top_edge: bfloat16 [96, 96, 36], P('row', 'col'), may hold values from -0.625 to 0.625
- right_edge: bfloat16 [96, 96, 36], P('row', 'col'), may hold values from -0.625 to 0.625
- bottom_edge: bfloat16 [96, 96, 36], P('row', 'col'), may hold values from -0.625 to 0.625
- left_edge: bfloat16 [96, 96, 36], P('row', 'col'), may hold values from -0.625 to 0.625
- site_tensor: bfloat16 [1679616], replicated, may hold values from -0.15625 to 0.15625
- top_projector: bfloat16 [3456, 96], P('col'), may hold values from -0.109375 to 0.109375
- bottom_projector: bfloat16 [3456, 96], P('col'), may hold values from -0.109375 to 0.109375
Outputs:
- upper_half: bfloat16 [3456, 3456], P('row', 'col')
- left_half: bfloat16 [3456, 3456], P('col', 'row')
- corner_top: bfloat16 [96, 3456], P('col', 'row')
- corner_bottom: bfloat16 [96, 3456], P('col', 'row')
The draws below stay inside these ranges and needn't reach their ends.
All inputs are finite; a program needn't handle non-finite values.
Results may differ from the reference program's by a relative error of at most 0.0081.
Values may be sent and summed in bfloat16 or wider, within the bound.
No kernel may reach another device: no remote copies, remote signals or barrier semaphores. Data moves between devices by JAX's collectives and lax.ppermute only.
A program may use at most 128 MiB of HBM per device.

```python
import jax
import jax.numpy as jnp

D = 6
CHI = 96
DD = 36
WIDE = 3456


def block_scale(stream_key, extent, cuts, least, largest):
    def one(axis_at, shards_of):
        heights = jax.random.uniform(jax.random.fold_in(jax.random.fold_in(stream_key, 6), axis_at), (shards_of,), jnp.float32, least / len(cuts), largest / len(cuts))
        return jnp.repeat(jnp.exp(heights), extent[axis_at] // shards_of).reshape((-1,) + (1,) * (len(extent) - axis_at - 1))

    gain = one(*cuts[0])
    for cut in cuts[1:]:
        gain = gain * one(*cut)
    return gain


def scatter_about(own_key, shape, spread, reach, split=(), kind=jnp.bfloat16):
    level = block_scale(own_key, shape, split, -0.22, 0.18) if split else 1.0
    values = jax.random.normal(own_key, shape, jnp.float32) * spread * level
    return jnp.minimum(jnp.maximum(values, -reach), reach).astype(kind)


def setup_inputs(seed: int = 0) -> dict:
    seeds = jax.random.split(jax.random.key(seed), 11)
    return {
        "upper_corner": scatter_about(seeds[0], (CHI, CHI), 1.0, 6.0, ((1, 16),)),
        "right_corner": scatter_about(seeds[1], (CHI, CHI), 1.0, 6.0, ((1, 16),)),
        "lower_corner": scatter_about(seeds[2], (CHI, CHI), 1.0, 6.0, ((1, 16),)),
        "top_edge": scatter_about(seeds[3], (CHI, CHI, DD), CHI ** -0.5, 0.625, ((0, 16), (1, 16))),
        "right_edge": scatter_about(seeds[4], (CHI, CHI, DD), CHI ** -0.5, 0.625, ((0, 16), (1, 16))),
        "bottom_edge": scatter_about(seeds[5], (CHI, CHI, DD), CHI ** -0.5, 0.625, ((0, 16), (1, 16))),
        "left_edge": scatter_about(seeds[6], (CHI, CHI, DD), CHI ** -0.5, 0.625, ((0, 16), (1, 16))),
        "site_tensor": scatter_about(seeds[7], (D ** 8,), (D ** 4) ** -0.5, 0.15625),
        "top_projector": scatter_about(seeds[8], (WIDE, CHI), WIDE ** -0.5, 0.109375, ((0, 16),)),
        "bottom_projector": scatter_about(seeds[9], (WIDE, CHI), WIDE ** -0.5, 0.109375, ((0, 16),)),
    }


def absorb(corner, edge):
    return jnp.einsum("cd,dbv->cbv", corner.astype(jnp.float32), edge.astype(jnp.float32)).astype(jnp.bfloat16)


def contract(form, first, second):
    return jnp.einsum(form, first.astype(jnp.float32), second.astype(jnp.float32)).astype(jnp.bfloat16)


def reference(upper_corner, right_corner, lower_corner, top_edge, right_edge, bottom_edge, left_edge, site_tensor, top_projector, bottom_projector):
    composite = CHI * D * D
    factor = composite ** -0.5
    double = D * D
    site = site_tensor.reshape(double, double, double, double)
    absorbed_top = absorb(upper_corner, top_edge)
    absorbed_right = absorb(right_corner, right_edge)
    absorbed_bottom = absorb(lower_corner, bottom_edge)
    partial_top = contract("acu,cbv->aubv", left_edge, absorbed_top)
    partial_right = contract("bdv,dgw->bvgw", top_edge, absorbed_right)
    partial_bottom = contract("cau,cbv->aubv", left_edge, absorbed_bottom)
    enlarged_top = contract("aubv,vust->asbt", partial_top, site).reshape(composite, composite)
    enlarged_right = contract("bvgw,vtsw->btgs", partial_right, site).reshape(composite, composite)
    enlarged_bottom = contract("aubv,suvt->asbt", partial_bottom, site).reshape(composite, composite)
    upper_half = (jnp.dot(enlarged_top, enlarged_right, preferred_element_type=jnp.float32) * factor).astype(jnp.bfloat16)
    left_half = (jnp.dot(enlarged_top.T, enlarged_bottom, preferred_element_type=jnp.float32) * factor).astype(jnp.bfloat16)
    corner_top = jnp.dot(top_projector.T, enlarged_top.T, preferred_element_type=jnp.float32).astype(jnp.bfloat16)
    corner_bottom = jnp.dot(bottom_projector.T, enlarged_bottom.T, preferred_element_type=jnp.float32).astype(jnp.bfloat16)
    return upper_half, left_half, corner_top, corner_bottom
```

```python
import jax
import jax.numpy as jnp
from jax import lax
from jax.experimental import pallas as pl
from jax.experimental.pallas import tpu as pltpu
from jax.sharding import PartitionSpec as P

F=jnp.float32; B=jnp.bfloat16
NN=(((1,),(0,)),((),()));NT=(((1,),(1,)),((),()))
def dot(x,y,dims=NN): return lax.dot_general(x,y,dims,preferred_element_type=F)
MCH=432
def expand(order_ref, buf_ref, off, dst):
    for rel in range(16):
        at=pl.multiple_of(order_ref[rel]*216,8)
        dst[pl.ds(at,216),:]=buf_ref[rel*496+off:rel*496+off+216,:].astype(F)
def to_bf16(src,dst):
    def f(i,_):
        at=pl.multiple_of(i*48,16)
        for a in range(6):
            dst[pl.ds(at,48),a*128:(a+1)*128]=src[a,pl.ds(at,48),:].astype(B)
        return 0
    lax.fori_loop(0,27,f,0)
def big(w_ref,p_ref,o_ref):
    def f(i,_):
        at=pl.multiple_of(i*MCH,16)
        res=dot(w_ref[pl.ds(at,MCH),:],p_ref[...])
        for a in range(6):
            o_ref[a,pl.ds(at,MCH),:]=res[:,a*128:(a+1)*128]
        return 0
    lax.fori_loop(0,1296//MCH,f,0)
    o_ref[:,1296:1440,:]=jnp.zeros((6,144,128),F)
def upper_kernel(order_ref, buf_ref, small_ref, wtop_ref, wright_ref, tpy_ref, out_ref, ct_ref, tef, pf, p1, p3, o1, o3):
    expand(order_ref, buf_ref, 0, tef)
    uc=small_ref[648:744,:]; rc=small_ref[744:840,:]
    ler=buf_ref[216:432,:]
    lu=dot(ler[:,:96],uc).astype(B)[:,:96]
    ar=dot(small_ref[216:432,:],rc,NT).astype(B)
    for v in range(36):
        te=tef[pl.ds(v,96,stride=36),:].astype(B)
        d1=dot(lu,te)
        for a in range(6):
            pf[a,v*36:(v+1)*36,:]=d1[a*36:(a+1)*36,:]
    to_bf16(pf,p1)
    for v in range(36):
        te=tef[pl.ds(v,96,stride=36),:].astype(B)
        d3=dot(ar,te[:,:96],NT)
        d3=jnp.concatenate([d3,jnp.zeros((216,32),F)],axis=1)
        for a in range(6):
            pf[a,v*36:(v+1)*36,:]=d3[a*36:(a+1)*36,:]
    to_bf16(pf,p3)
    big(wtop_ref,p1,o1)
    big(wright_ref,p3,o3)
    acc=jnp.zeros((240,248),F)
    for tp in range(18):
        xs=[];ys=[]
        for t in (2*tp,2*tp+1):
            xs.append(jnp.concatenate([o1[a,pl.ds(t,40,stride=36),:] for a in range(6)],axis=0).astype(B))
            ys.append(jnp.concatenate([o3[g,pl.ds(t,40,stride=36),:] for g in range(6)]+[tpy_ref[t*8:(t+1)*8,:].astype(F)],axis=0).astype(B))
        acc=acc+dot(jnp.concatenate(xs,axis=1),jnp.concatenate(ys,axis=1),NT)
    fac=jnp.float32(3456.0**-0.5)
    up=(acc[:,:240]*fac)
    for a in range(6):
        for g in range(6):
            out_ref[a*36:(a+1)*36,g*36:(g+1)*36]=up[a*40:a*40+36,g*40:g*40+36].astype(B)
    ct_ref[...]=acc[:,240:248]
def left_kernel(order_ref, buf_ref, small_ref, ber_ref, wtop_ref, wbot_ref, bpr_ref, out_ref, cb_ref, lef, pf, p2, p4, o2, o4):
    expand(order_ref, buf_ref, 216, lef)
    uc=small_ref[648:744,:]; lc=small_ref[840:936,:]
    at=dot(small_ref[0:216,:],uc,NT).astype(B)
    ab=dot(ber_ref[...],lc,NT).astype(B)
    for u in range(36):
        le=lef[pl.ds(u,96,stride=36),:].astype(B)
        d2=dot(at,le[:,:96],NT)
        d2=jnp.concatenate([d2,jnp.zeros((216,32),F)],axis=1)
        for b in range(6):
            pf[b,pl.ds(u,36,stride=36),:]=d2[b*36:(b+1)*36,:]
    to_bf16(pf,p2)
    for u in range(36):
        le=lef[pl.ds(u,96,stride=36),:].astype(B)
        d4=dot(ab,le)
        for b in range(6):
            pf[b,pl.ds(u,36,stride=36),:]=d4[b*36:(b+1)*36,:]
    to_bf16(pf,p4)
    big(wtop_ref,p2,o2)
    big(wbot_ref,p4,o4)
    acc=jnp.zeros((240,240),F)
    for sp in range(18):
        xs=[];ys=[]
        for s in (2*sp,2*sp+1):
            x=jnp.concatenate([o2[b,s*36:s*36+40,:] for b in range(6)],axis=0).astype(B)
            y=jnp.concatenate([o4[b,s*36:s*36+40,:] for b in range(6)],axis=0).astype(B)
            xs.append(x);ys.append(y)
            cb_ref[s*8:(s+1)*8,:]=dot(bpr_ref[...],y)
        acc=acc+dot(jnp.concatenate(xs,axis=1),jnp.concatenate(ys,axis=1),NT)
    lh=acc*jnp.float32(3456.0**-0.5)
    for a in range(6):
        for g in range(6):
            out_ref[a*36:(a+1)*36,g*36:(g+1)*36]=lh[a*40:a*40+36,g*40:g*40+36].astype(B)
VM=pl.BlockSpec(memory_space=pltpu.VMEM); SM=pl.BlockSpec(memory_space=pltpu.SMEM)
def scr(): return [pltpu.VMEM((3456,128),F),pltpu.VMEM((6,1296,128),F),pltpu.VMEM((1296,768),B),pltpu.VMEM((1296,768),B),pltpu.VMEM((6,1440,128),F),pltpu.VMEM((6,1440,128),F)]
def upper(order,buf,small,wtop,wright,tpy):
    return pl.pallas_call(upper_kernel,out_shape=(jax.ShapeDtypeStruct((216,216),B),jax.ShapeDtypeStruct((240,8),F)),
        in_specs=[SM]+[VM]*5,out_specs=(VM,VM),scratch_shapes=scr(),name="upper",
        compiler_params=pltpu.CompilerParams(vmem_limit_bytes=56<<20))(order,buf,small,wtop,wright,tpy)
def left(order,buf,small,ber,wtop,wbot,bpr):
    return pl.pallas_call(left_kernel,out_shape=(jax.ShapeDtypeStruct((216,216),B),jax.ShapeDtypeStruct((288,128),F)),
        in_specs=[SM]+[VM]*6,out_specs=(VM,VM),scratch_shapes=scr(),name="left",
        compiler_params=pltpu.CompilerParams(vmem_limit_bytes=56<<20))(order,buf,small,ber,wtop,wbot,bpr)


def lanes_shifted(a_ref, z_ref, pair):
    tile = (pair * 72) // 128
    base = pl.multiple_of(tile * 128, 128)
    off = pair * 72 - tile * 128
    k = lax.broadcasted_iota(jnp.int32, (256, 256), 0)
    n = lax.broadcasted_iota(jnp.int32, (256, 256), 1)
    w = n % 128
    sel = ((k == off + (n // 128) * 36 + w) & (w < 36)).astype(B)
    z_ref[...] = dot(a_ref[:, pl.ds(base, 256)], sel)
def realign(a_ref, z_ref, o_ref):
    def f(g, _):
        strips = []
        for h in range(2):
            lanes_shifted(a_ref, z_ref.at[h], 2 * g + h)
            for q in range(2):
                strips.append(jnp.concatenate([z_ref[h, k * 36:(k + 1) * 36, q * 128:q * 128 + 36] for k in range(36)], axis=1))
        at = pl.multiple_of(g * 144, 16)
        o_ref[pl.ds(at, 144), :] = jnp.concatenate(strips, axis=0).astype(B)
        return 0
    lax.fori_loop(0, 9, f, 0)
def site_kernel(s_ref, wtop_ref, wright_ref, wbot_ref, apad, z):
    zero = jnp.zeros((1296, 112), B)
    apad[:, 1296:1408] = zero
    apad[:, :1296] = s_ref[...]
    realign(apad, z, wright_ref)
    eye = (lax.broadcasted_iota(jnp.int32, (128, 128), 0) == lax.broadcasted_iota(jnp.int32, (128, 128), 1)).astype(B)
    for b in range(11):
        res = dot(eye, apad[:, b * 128:(b + 1) * 128], NT).astype(B)
        n = min(128, 1296 - b * 128)
        wtop_ref[b * 128:b * 128 + n, :] = res[:n]
    apad[:, :1296] = wtop_ref[...]
    realign(apad, z, wbot_ref)
def site_forms(s2):
    shape = jax.ShapeDtypeStruct((1296, 1296), B)
    return pl.pallas_call(site_kernel, out_shape=(shape,) * 3, in_specs=[VM], out_specs=(VM,) * 3,
        scratch_shapes=[pltpu.VMEM((1296, 1408), B), pltpu.VMEM((2, 1296, 256), F)], name="site",
        compiler_params=pltpu.CompilerParams(vmem_limit_bytes=56 << 20))(s2)

ROW, COL = "row", "col"


def row_permute(x, move):
    pairs = []
    for y in range(4):
        for z in range(2):
            for k in range(2):
                a, b, c = move(y, z, k)
                pairs.append((y * 4 + z * 2 + k, a * 4 + b * 2 + c))
    return lax.ppermute(x, ROW, pairs)


def col_permute(x, move):
    pairs = []
    for z in range(4):
        for i in range(4):
            a, b = move(z, i)
            pairs.append((z * 4 + i, a * 4 + b))
    return lax.ppermute(x, COL, pairs)


def swap_axes(x):
    pairs = [(r * 16 + c, c * 16 + r) for r in range(16) for c in range(16)]
    return lax.ppermute(x, (ROW, COL), pairs)


def stacked(own, received):
    return jnp.concatenate([own, *received], axis=0)


def shards(uc, rc, lc, te, re, be, le, site_flat, tp, bp):
    bf = jnp.bfloat16
    r = lax.axis_index(ROW)
    c = lax.axis_index(COL)
    y, zlo, core = r // 4, (r // 2) % 2, r % 2
    zhi, x = c // 4, c % 4

    tp_send = tp.reshape(216, 16, 6).transpose(1, 2, 0)
    tp_all = lax.all_to_all(tp_send, COL, 0, 0, tiled=True)
    tpy = tp_all.reshape(16, 6, 6, 36).transpose(3, 1, 0, 2).reshape(36, 6, 96)
    tpy = jnp.pad(tpy, ((0, 0), (0, 2), (0, 32))).reshape(288, 128)
    bp_row = swap_axes(bp)
    bpr = lax.dynamic_slice_in_dim(bp_row, c * 6, 6, 1).T.reshape(6, 6, 36)
    bpr = jnp.pad(bpr, ((0, 2), (0, 0), (0, 4))).reshape(8, 240)

    side = lambda e: jnp.pad(e.transpose(1, 0, 2).reshape(6, 216), ((0, 2), (0, 0)))
    piece = jnp.concatenate([side(te), side(le)], axis=0)
    piece = stacked(piece, [col_permute(piece, lambda z, i, s=s: ((z + s) % 4, i)) for s in (1, 2, 3)])
    piece = stacked(piece, [col_permute(piece, lambda z, i, s=s: (z, (i + s) % 4)) for s in (1, 2, 3)])
    at = jnp.arange(256)
    x_rel, z_rel, edge, j = at // 64, (at // 16) % 4, (at // 8) % 2, at % 8
    block = ((zhi - z_rel) % 4) * 4 + (x - x_rel) % 4
    target = jnp.where(j < 6, edge * 128 + block * 6 + j, -1)
    place = (target[:, None] == jnp.arange(256)[None, :]).astype(bf)
    rows = lax.dot_general(piece, place, (((0,), (0,)), ((), ())), preferred_element_type=jnp.float32).astype(bf)

    pack = jnp.concatenate([te.reshape(6, 216), re.reshape(6, 216), be.reshape(6, 216), uc.T, rc.T, lc.T], axis=1)
    pack = jnp.pad(pack, ((0, 2), (0, 88)))
    pack = pack.reshape(8, 8, 128).transpose(1, 0, 2).reshape(64, 128)
    buf = jnp.concatenate([rows[:, :128], rows[:, 128:], pack], axis=0)
    buf = stacked(buf, [row_permute(buf, lambda a, b, k: (a, 1 - b, k))])
    buf = stacked(buf, [row_permute(buf, lambda a, b, k, s=s: ((a + s) % 4, b, k)) for s in (1, 2, 3)])
    buf = stacked(buf, [row_permute(buf, lambda a, b, k: (a, b, 1 - k))])
    rel = jnp.arange(16)
    order = ((y - (rel // 2) % 4) % 4) * 4 + (zlo ^ (rel % 2)) * 2 + (core ^ (rel // 8))
    order = order.astype(jnp.int32)

    packs = buf.reshape(16, 496, 128)[:, 432:].reshape(16, 8, 8, 128).transpose(0, 2, 1, 3).reshape(128, 1024)
    at = jnp.arange(128)
    target = jnp.where(at % 8 < 6, jnp.repeat(order, 8) * 6 + at % 8, -1)
    place = (target[:, None] == jnp.arange(128)[None, :]).astype(bf)
    small = lax.dot_general(packs, place, (((0,), (0,)), ((), ())), preferred_element_type=jnp.float32).astype(bf)
    ber = swap_axes(small[432:648])

    wtop, wright, wbot = site_forms(site_flat.reshape(1296, 1296))

    up, ct = upper(order, buf, small, wtop, wright, tpy)
    lf, cb = left(order, buf, small, ber, wtop, wbot, bpr)
    corner_top = ct.reshape(6, 40, 8)[:, :36, :6].reshape(216, 6).T.astype(bf)
    part = cb.reshape(36, 8, 128)[:, :6, :96].reshape(36, 6, 16, 6).transpose(2, 1, 3, 0).reshape(16, 6, 216)
    corner_bottom = jnp.sum(lax.all_to_all(part, ROW, 0, 0, tiled=True), axis=0).astype(bf)
    return up, lf, corner_top, corner_bottom


def solution(mesh):
    placed = (
        P(None, ROW),
        P(None, ROW),
        P(None, ROW),
        P(ROW, COL, None),
        P(ROW, COL, None),
        P(ROW, COL, None),
        P(ROW, COL, None),
        P(),
        P(COL, None),
        P(COL, None),
    )
    return jax.shard_map(
        shards,
        mesh=mesh,
        in_specs=placed,
        out_specs=(P(ROW, COL), P(COL, ROW), P(COL, ROW), P(COL, ROW)),
        check_vma=False,
    )
```

```python
import jax
import jax.numpy as jnp
from jax import lax
from jax.experimental import pallas as pl
from jax.experimental.pallas import tpu as pltpu
from jax.sharding import PartitionSpec as P

F = jnp.float32
B = jnp.bfloat16
NN = (((1,), (0,)), ((), ()))
NT = (((1,), (1,)), ((), ()))
VM = pl.BlockSpec(memory_space=pltpu.VMEM)
SM = pl.BlockSpec(memory_space=pltpu.SMEM)
BLOCK = 512
WIDE = 3456


def dot(x, y, dims=NN):
    return lax.dot_general(x, y, dims, preferred_element_type=F)


def shape_of(*dims, kind=B):
    return jax.ShapeDtypeStruct(dims, kind)


def params(mib):
    return pltpu.CompilerParams(vmem_limit_bytes=mib << 20)


def work(flops):
    return pl.CostEstimate(flops=flops, transcendentals=0, bytes_accessed=1 << 22)


def prepare_kernel(te, re, be, le, uct, rct, lct, piece, pack):
    zero = jnp.zeros((2, 216), B)
    for n, e in ((0, te), (1, le)):
        v = e[...].astype(F)
        piece[8 * n:8 * n + 8, :] = jnp.concatenate(
            [jnp.concatenate([v[i] for i in range(6)], axis=1).astype(B), zero], axis=0)
    parts = []
    for e in (te, re, be):
        v = e[...].astype(F)
        parts.append(jnp.concatenate([v[:, j, :] for j in range(6)], axis=1))
    for c in (uct, rct, lct):
        parts.append(c[...].astype(F))
    flat = jnp.concatenate(parts + [jnp.zeros((6, 88), F)], axis=1)
    flat = jnp.concatenate([flat, jnp.zeros((2, 1024), F)], axis=0).astype(B)
    for k in range(8):
        pack[8 * k:8 * k + 8, :] = flat[:, 128 * k:128 * k + 128]


def expand(order_ref, bufs, off, dst):
    for rel in range(16):
        at = pl.multiple_of(order_ref[rel] * 216, 8)
        start = (rel % 2) * BLOCK + off
        dst[pl.ds(at, 216), :] = bufs[rel // 2][start:start + 216, :].astype(F)


def gather_small_kernel(order_ref, *refs):
    bufs = refs[:8]
    out_ref, packs = refs[8:]
    for rel in range(16):
        at = pl.multiple_of(order_ref[rel] * 8, 8)
        start = (rel % 2) * BLOCK + 432
        for k in range(10):
            packs[k, pl.ds(at, 8), :] = bufs[rel // 2][start + 8 * k:start + 8 * k + 8, :].astype(F)
    row = lax.broadcasted_iota(jnp.int32, (128, 128), 0)
    lane = lax.broadcasted_iota(jnp.int32, (128, 128), 1)
    place = ((row % 8 < 6) & (lane == (row // 8) * 6 + row % 8)).astype(B)
    for k in range(10):
        out_ref[k * 128:(k + 1) * 128, :] = dot(jnp.transpose(packs[k]).astype(B), place).astype(B)


def gather_small(order, bufs):
    return pl.pallas_call(gather_small_kernel, out_shape=shape_of(1280, 128), in_specs=[SM] + [VM] * 8, out_specs=VM,
                          scratch_shapes=[pltpu.VMEM((10, 128, 128), F)], name="gather_small",
                          compiler_params=params(6))(order, *bufs)


def to_bf16(src, dst, rows):
    def f(i, _):
        at = pl.multiple_of(i * 48, 16)
        for a in range(6):
            dst[pl.ds(at, 48), a * 128:(a + 1) * 128] = src[a, pl.ds(at, 48), :].astype(B)
        return 0
    lax.fori_loop(0, rows // 48, f, 0)


def big(w_ref, p_ref, k, o_ref):
    def f(i, _):
        at = pl.multiple_of(i * 432, 16)
        res = dot(w_ref[pl.ds(at, 432), :], p_ref[:k, :])
        for a in range(6):
            o_ref[a, pl.ds(at, 432), :] = res[:, a * 128:(a + 1) * 128]
        return 0
    lax.fori_loop(0, 3, f, 0)
    o_ref[:, 1296:1440, :] = jnp.zeros((6, 144, 128), F)


def padded(x):
    return jnp.concatenate([x, jnp.zeros((x.shape[0], 32), F)], axis=1)


def clear_gaps(pf):
    for q in range(12):
        pf[:, q * 128 + 108:(q + 1) * 128, :] = jnp.zeros((6, 20, 128), F)


def compressed(x):
    return jnp.concatenate([x[:, g * 40:g * 40 + 36] for g in range(6)], axis=1)


def upper_kernel(order_ref, *refs):
    bufs = refs[:8]
    small_ref, wtop_ref, wright_ref, out_ref, ct_ref, tef, pf, p1, p3, o1, o3, tps = refs[8:]
    expand(order_ref, bufs, 0, tef)
    uc = small_ref[648:744, :]
    rc = small_ref[744:840, :]
    tps[0:216, :] = small_ref[1024:1240, :].astype(F)
    tps[216:320, :] = jnp.zeros((104, 128), F)
    lu = dot(bufs[0][216:432, :][:, :96], uc).astype(B)[:, :96]
    ar = dot(small_ref[216:432, :], rc, NT).astype(B)
    for v in range(36):
        te = tef[pl.ds(v, 96, stride=36), :].astype(B)
        d1 = dot(lu, te)
        for a in range(6):
            pf[a, v * 36:(v + 1) * 36, :] = d1[a * 36:(a + 1) * 36, :]
    to_bf16(pf, p1, 1296)
    clear_gaps(pf)
    for v in range(36):
        te = tef[pl.ds(v, 96, stride=36), :].astype(B)
        d3 = padded(dot(ar, te[:, :96], NT))
        at = (v // 3) * 128 + (v % 3) * 36
        for a in range(6):
            pf[a, at:at + 36, :] = d3[a * 36:(a + 1) * 36, :]
    to_bf16(pf, p3, 1536)
    big(wtop_ref, p1, 1296, o1)
    big(wright_ref, p3, 1536, o3)
    acc = jnp.zeros((240, 256), F)
    for tp in range(18):
        xs = []
        ys = []
        for t in (2 * tp, 2 * tp + 1):
            xs.append(jnp.concatenate([o1[a, pl.ds(t, 40, stride=36), :] for a in range(6)], axis=0).astype(B))
            ys.append(jnp.concatenate([o3[g, pl.ds(t, 40, stride=36), :] for g in range(6)]
                                      + [tps[pl.ds(t, 8, stride=36), :], jnp.zeros((8, 128), F)], axis=0).astype(B))
        acc = acc + dot(jnp.concatenate(xs, axis=1), jnp.concatenate(ys, axis=1), NT)
    up = compressed(acc[:, :240] * jnp.float32(WIDE ** -0.5))
    for a in range(6):
        out_ref[a * 36:(a + 1) * 36, :] = up[a * 40:a * 40 + 36, :].astype(B)
    ct = jnp.transpose(acc[:, 128:256])[112:120, :]
    ct_ref[...] = compressed(ct)[0:6, :].astype(B)


def left_kernel(order_ref, *refs):
    bufs = refs[:8]
    small_ref, ber_ref, wtop_ref, wbot_ref, bpr_ref, out_ref, cb_ref, lef, pf, p2, p4, o2, o4, cbs, abf = refs[8:]
    expand(order_ref, bufs, 216, lef)
    uc = small_ref[648:744, :]
    lc = small_ref[840:936, :]
    at = dot(small_ref[0:216, :], uc, NT).astype(B)
    abf[...] = padded(dot(ber_ref[...], lc, NT))
    ab = jnp.concatenate([abf[pl.ds(b * 36 + h, 12, stride=3), :] for b in range(6) for h in range(3)], axis=0).astype(B)[:, :96]
    for u in range(36):
        le = lef[pl.ds(u, 96, stride=36), :].astype(B)
        d2 = padded(dot(at, le[:, :96], NT))
        for b in range(6):
            pf[b, pl.ds(u, 36, stride=36), :] = d2[b * 36:(b + 1) * 36, :]
    to_bf16(pf, p2, 1296)
    clear_gaps(pf)
    for u in range(36):
        le = lef[pl.ds(u, 96, stride=36), :].astype(B)
        d4 = dot(ab, le)
        for b in range(6):
            for h in range(3):
                pf[b, pl.ds(h * 36 + u, 12, stride=128), :] = d4[b * 36 + h * 12:b * 36 + h * 12 + 12, :]
    to_bf16(pf, p4, 1536)
    big(wtop_ref, p2, 1296, o2)
    big(wbot_ref, p4, 1536, o4)
    acc = jnp.zeros((240, 240), F)
    for sp in range(18):
        xs = []
        ys = []
        for s in (2 * sp, 2 * sp + 1):
            x = jnp.concatenate([o2[b, s * 36:s * 36 + 40, :] for b in range(6)], axis=0).astype(B)
            y = jnp.concatenate([o4[b, s * 36:s * 36 + 40, :] for b in range(6)], axis=0).astype(B)
            xs.append(x)
            ys.append(y)
            cbs[pl.ds(s, 8, stride=36), :] = dot(bpr_ref[...], y)
        acc = acc + dot(jnp.concatenate(xs, axis=1), jnp.concatenate(ys, axis=1), NT)
    lh = compressed(acc * jnp.float32(WIDE ** -0.5))
    for a in range(6):
        out_ref[a * 36:(a + 1) * 36, :] = lh[a * 40:a * 40 + 36, :].astype(B)
    cb_ref[...] = cbs[0:216, :]


def scratch():
    return [pltpu.VMEM((WIDE, 128), F), pltpu.VMEM((6, 1536, 128), F), pltpu.VMEM((1536, 768), B),
            pltpu.VMEM((1536, 768), B), pltpu.VMEM((6, 1440, 128), F), pltpu.VMEM((6, 1440, 128), F)]


def prepare(te, re, be, le, uct, rct, lct):
    return pl.pallas_call(prepare_kernel, out_shape=(shape_of(16, 216), shape_of(64, 128)), in_specs=[VM] * 7,
                          out_specs=(VM, VM), name="prepare", compiler_params=params(4))(te, re, be, le, uct, rct, lct)


def upper(order, bufs, small, wtop, wright):
    return pl.pallas_call(
        upper_kernel, out_shape=(shape_of(216, 216), shape_of(6, 216)), in_specs=[SM] + [VM] * 11, out_specs=(VM, VM),
        scratch_shapes=scratch() + [pltpu.VMEM((320, 128), F)], name="upper", compiler_params=params(23),
        cost_estimate=work(8 << 30))(order, *bufs, small, wtop, wright)


def left(order, bufs, small, ber, wtop, wbot, bpr):
    return pl.pallas_call(
        left_kernel, out_shape=(shape_of(216, 216), shape_of(216, 128, kind=F)), in_specs=[SM] + [VM] * 13,
        out_specs=(VM, VM), scratch_shapes=scratch() + [pltpu.VMEM((288, 128), F), pltpu.VMEM((216, 128), F)], name="left",
        compiler_params=params(23), cost_estimate=work(8 << 30))(order, *bufs, small, ber, wtop, wbot, bpr)


def finish_kernel(at_ref, own, one, two, three, out_ref):
    total = (own[...] + one[...] + two[...] + three[...]).astype(B)
    lane = lax.broadcasted_iota(jnp.int32, (8, 128), 1)
    pick = (lane == at_ref[0] + lax.broadcasted_iota(jnp.int32, (8, 128), 0)).astype(B)
    res = dot(pick, total, NT)
    rows = [jnp.concatenate([res[a:a + 1, x * 36:(x + 1) * 36] for a in range(6)], axis=1) for x in range(6)]
    out_ref[...] = jnp.concatenate(rows, axis=0).astype(B)


def finish(at, *parts):
    return pl.pallas_call(finish_kernel, out_shape=shape_of(6, 216), in_specs=[SM] + [VM] * 4, out_specs=VM,
                          name="finish", compiler_params=params(4))(at, *parts)


def lanes_shifted(a_ref, z_ref, pair):
    tile = (pair * 72) // 128
    base = pl.multiple_of(tile * 128, 128)
    off = pair * 72 - tile * 128
    k = lax.broadcasted_iota(jnp.int32, (256, 256), 0)
    n = lax.broadcasted_iota(jnp.int32, (256, 256), 1)
    w = n % 128
    sel = ((k == off + (n // 128) * 36 + w % 36) & (w < 108)).astype(B)
    z_ref[...] = dot(a_ref[:, pl.ds(base, 256)], sel)


def realign(a_ref, z_ref, o_ref):
    lane = lax.broadcasted_iota(jnp.int32, (36, 128), 1)

    def f(g, _):
        strips = []
        for h in range(2):
            lanes_shifted(a_ref, z_ref.at[h], 2 * g + h)
        for h in range(2):
            for q in range(2):
                tiles = []
                for m in range(12):
                    z = [z_ref[h, (3 * m + e) * 36:(3 * m + e + 1) * 36, q * 128:(q + 1) * 128] for e in range(3)]
                    tiles.append(jnp.where(lane < 36, z[0], jnp.where(lane < 72, z[1], z[2])))
                strips.append(jnp.concatenate(tiles, axis=1))
        at = pl.multiple_of(g * 144, 16)
        o_ref[pl.ds(at, 144), :] = jnp.concatenate(strips, axis=0).astype(B)
        return 0
    lax.fori_loop(0, 9, f, 0)


def right_form_kernel(s_ref, wright_ref, apad, z):
    apad[:, 1296:1408] = jnp.zeros((1296, 112), B)
    apad[:, :1296] = s_ref[...]
    realign(apad, z, wright_ref)


def left_forms_kernel(s_ref, wtop_ref, wbot_ref, apad, z):
    eye = (lax.broadcasted_iota(jnp.int32, (128, 128), 0) == lax.broadcasted_iota(jnp.int32, (128, 128), 1)).astype(B)
    for b in range(11):
        n = min(128, 1296 - b * 128)
        res = dot(eye[:n, :n], s_ref[:, b * 128:b * 128 + n], NT).astype(B)
        wtop_ref[b * 128:b * 128 + n, :] = res
        apad[b * 128:b * 128 + n, :1296] = res
    apad[:, 1296:1408] = jnp.zeros((1296, 112), B)
    realign(apad, z, wbot_ref)


def form_scratch():
    return [pltpu.VMEM((1296, 1408), B), pltpu.VMEM((2, 1296, 256), F)]


def right_form(s2):
    return pl.pallas_call(right_form_kernel, out_shape=shape_of(1296, 1536), in_specs=[VM], out_specs=VM,
                          scratch_shapes=form_scratch(), name="right_form", compiler_params=params(9),
                          cost_estimate=work(3 << 30))(s2)


def left_forms(s2):
    return pl.pallas_call(left_forms_kernel, out_shape=(shape_of(1296, 1296), shape_of(1296, 1536)), in_specs=[VM],
                          out_specs=(VM, VM), scratch_shapes=form_scratch(), name="left_forms", compiler_params=params(9),
                          cost_estimate=work(4 << 30))(s2)


ROW, COL = "row", "col"


def row_permute(x, move):
    pairs = []
    for y in range(4):
        for z in range(2):
            for k in range(2):
                a, b, c = move(y, z, k)
                pairs.append((y * 4 + z * 2 + k, a * 4 + b * 2 + c))
    return lax.ppermute(x, ROW, pairs)


def col_permute(x, move):
    pairs = []
    for z in range(4):
        for i in range(4):
            a, b = move(z, i)
            pairs.append((z * 4 + i, a * 4 + b))
    return lax.ppermute(x, COL, pairs)


def swap_axes(x):
    pairs = [(r * 16 + c, c * 16 + r) for r in range(16) for c in range(16)]
    return lax.ppermute(x, (ROW, COL), pairs)


def stacked(own, received):
    return jnp.concatenate([own, *received], axis=0)


def other_core(x):
    return row_permute(x, lambda a, b, k: (a, b, 1 - k))


def other_z(x):
    return row_permute(x, lambda a, b, k: (a, 1 - b, k))


def along_y(x, s):
    return row_permute(x, lambda a, b, k: ((a + s) % 4, b, k))


def shards(uc, rc, lc, te, re, be, le, site_flat, tp, bp):
    r = lax.axis_index(ROW)
    c = lax.axis_index(COL)
    y, zlo, core = r // 4, (r // 2) % 2, r % 2
    zhi, x = c // 4, c % 4
    hold = lax.optimization_barrier

    piece, pack = prepare(te, re, be, le, uc.T, rc.T, lc.T)
    s2 = site_flat.reshape(1296, 1296)

    projectors = swap_axes(jnp.concatenate([tp, bp], axis=1))

    got = [col_permute(piece, lambda z, i, s=s: ((z + s) % 4, i)) for s in (1, 2, 3)]
    *got, s2 = hold((*got, s2))
    piece = stacked(piece, got)
    piece = stacked(piece, [col_permute(piece, lambda z, i, s=s: (z, (i + s) % 4)) for s in (1, 2, 3)])
    at = jnp.arange(256)
    x_rel, z_rel, edge, j = at // 64, (at // 16) % 4, (at // 8) % 2, at % 8
    block = ((zhi - z_rel) % 4) * 4 + (x - x_rel) % 4
    target = jnp.where(j < 6, edge * 128 + block * 6 + j, -1)
    place = (target[:, None] == jnp.arange(256)[None, :]).astype(B)
    rows = lax.dot_general(piece, place, (((0,), (0,)), ((), ())), preferred_element_type=F).astype(B)

    tpx = lax.dynamic_slice_in_dim(projectors, c * 6, 6, 1)
    tpx = tpx.reshape(6, 36, 6).transpose(0, 2, 1).reshape(6, 216)
    tpx = jnp.pad(tpx, ((0, 2), (0, 40))).reshape(8, 2, 128).transpose(1, 0, 2).reshape(16, 128)
    bpr = lax.dynamic_slice_in_dim(projectors, 96 + c * 6, 6, 1).T.reshape(6, 6, 36)
    bpr = jnp.pad(bpr, ((0, 2), (0, 0), (0, 4))).reshape(8, 240)
    own = jnp.concatenate([rows[:, :128], rows[:, 128:], pack, tpx], axis=0)
    near = stacked(own, [other_z(own)])
    far = [along_y(near, s) for s in (1, 2, 3)]
    near_twin = other_core(near)
    wtop, wbot = left_forms(hold((s2, near))[0])
    *far, near_twin, wtop = hold((*far, near_twin, wtop))
    far_twin = [other_core(f) for f in far]
    bufs = [near, *far, near_twin, *far_twin]
    rel = jnp.arange(16)
    order = ((y - (rel // 2) % 4) % 4) * 4 + (zlo ^ (rel % 2)) * 2 + (core ^ (rel // 8))
    order = order.astype(jnp.int32)

    small = gather_small(order, bufs)
    ber = swap_axes(small[432:648])

    lf, cb = left(order, bufs, small, ber, wtop, wbot, bpr)
    cb = cb + other_core(cb)
    cb_z = other_z(cb)
    wright = right_form(hold((s2, cb))[0])
    cb_z, wright = hold((cb_z, wright))
    cb = cb + cb_z
    cb_y = [along_y(cb, s) for s in (1, 2, 3)]
    order = hold((order, cb))[0]
    up, corner_top = upper(order, bufs, small, wtop, wright)
    *cb_y, up = hold((*cb_y, up))
    corner_bottom = finish((r * 6).astype(jnp.int32).reshape(1), cb, *cb_y)
    return up, lf, corner_top, corner_bottom


def solution(mesh):
    placed = (
        P(None, ROW),
        P(None, ROW),
        P(None, ROW),
        P(ROW, COL, None),
        P(ROW, COL, None),
        P(ROW, COL, None),
        P(ROW, COL, None),
        P(),
        P(COL, None),
        P(COL, None),
    )
    return jax.shard_map(
        shards,
        mesh=mesh,
        in_specs=placed,
        out_specs=(P(ROW, COL), P(COL, ROW), P(COL, ROW), P(COL, ROW)),
        check_vma=False,
    )
```

```python
import jax
import jax.numpy as jnp
from jax import lax
from jax.experimental import pallas as pl
from jax.experimental.pallas import tpu as pltpu
from jax.sharding import PartitionSpec as P

F = jnp.float32
B = jnp.bfloat16
NN = (((1,), (0,)), ((), ()))
NT = (((1,), (1,)), ((), ()))
VM = pl.BlockSpec(memory_space=pltpu.VMEM)
SM = pl.BlockSpec(memory_space=pltpu.SMEM)
HB = pl.BlockSpec(memory_space=pltpu.HBM)
BLOCK = 512
WIDE = 3456


def dot(x, y, dims=NN):
    return lax.dot_general(x, y, dims, preferred_element_type=F)


def shape_of(*dims, kind=B):
    return jax.ShapeDtypeStruct(dims, kind)


def params(mib):
    return pltpu.CompilerParams(vmem_limit_bytes=mib << 20)


def work(flops):
    return pl.CostEstimate(flops=flops, transcendentals=0, bytes_accessed=1 << 22)


def load(pairs, sems):
    copies = [pltpu.make_async_copy(src, dst, sems.at[n]) for n, (src, dst) in enumerate(pairs)]
    for cp in copies:
        cp.start()
    return copies


def prepare_kernel(*refs):
    hbm, (piece, pack, turned), local, sems = refs[:9], refs[9:12], refs[12:21], refs[21]
    for cp in load(list(zip(hbm, local)), sems):
        cp.wait()
    te, re, be, le, uct, rct, lct, tpt, bpt = local
    zero = jnp.zeros((2, 216), B)
    for n, e in ((0, te), (1, le)):
        v = e[...].astype(F)
        piece[8 * n:8 * n + 8, :] = jnp.concatenate(
            [jnp.concatenate([v[i] for i in range(6)], axis=1).astype(B), zero], axis=0)
    parts = []
    for e in (te, re, be):
        v = e[...].astype(F)
        parts.append(jnp.concatenate([v[:, j, :] for j in range(6)], axis=1))
    turned[0:96, :] = tpt[...]
    turned[96:192, :] = bpt[...]
    turned[192:200, :] = jnp.concatenate([parts[2].astype(B), zero], axis=0)
    for c in (uct, rct, lct):
        parts.append(c[...].astype(F))
    flat = jnp.concatenate(parts + [jnp.zeros((6, 88), F)], axis=1)
    flat = jnp.concatenate([flat, jnp.zeros((2, 1024), F)], axis=0).astype(B)
    for k in range(8):
        pack[8 * k:8 * k + 8, :] = flat[:, 128 * k:128 * k + 128]


def pieces_kernel(at_ref, turned, piece, out, tpx, bpr):
    out[0:16, :] = piece[...]
    out[16:24, :] = turned[192:200, :]
    row = lax.broadcasted_iota(jnp.int32, (8, 96), 0)
    lane = lax.broadcasted_iota(jnp.int32, (8, 96), 1)
    pick = ((lane == at_ref[0] + row) & (row < 6)).astype(B)
    top = dot(pick, turned[0:96, :])
    flat = jnp.concatenate(
        [jnp.concatenate([top[x:x + 1, b * 36:(b + 1) * 36] for x in range(6)], axis=1) for b in range(6)], axis=0)
    flat = jnp.concatenate([flat, jnp.zeros((6, 40), F)], axis=1)
    flat = jnp.concatenate([flat, jnp.zeros((2, 256), F)], axis=0).astype(B)
    tpx[0:8, :] = flat[:, :128]
    tpx[8:16, :] = flat[:, 128:]
    bottom = dot(pick, turned[96:192, :])
    gap = jnp.zeros((8, 4), F)
    bpr[...] = jnp.concatenate([y for b in range(6) for y in (bottom[:, b * 36:(b + 1) * 36], gap)], axis=1).astype(B)


def expand(order_ref, bufs, off, dst):
    for rel in range(16):
        at = pl.multiple_of(order_ref[rel] * 216, 8)
        start = (rel % 2) * BLOCK + off
        dst[pl.ds(at, 216), :] = bufs[rel // 2][start:start + 216, :].astype(F)


def gather_small_kernel(order_ref, *refs):
    bufs = refs[:8]
    out_ref, packs = refs[8:]
    for rel in range(16):
        at = pl.multiple_of(order_ref[rel] * 8, 8)
        start = (rel % 2) * BLOCK + 432
        for k in range(10):
            packs[k, pl.ds(at, 8), :] = bufs[rel // 2][start + 8 * k:start + 8 * k + 8, :].astype(F)
    row = lax.broadcasted_iota(jnp.int32, (128, 128), 0)
    lane = lax.broadcasted_iota(jnp.int32, (128, 128), 1)
    place = ((row % 8 < 6) & (lane == (row // 8) * 6 + row % 8)).astype(B)
    for k in range(10):
        out_ref[k * 128:(k + 1) * 128, :] = dot(jnp.transpose(packs[k]).astype(B), place).astype(B)


def gather_small(order, bufs):
    return pl.pallas_call(gather_small_kernel, out_shape=shape_of(1280, 128), in_specs=[SM] + [VM] * 8, out_specs=VM,
                          scratch_shapes=[pltpu.VMEM((10, 128, 128), F)], name="gather_small",
                          compiler_params=params(6))(order, *bufs)


def to_bf16(src, dst, rows):
    def f(i, _):
        at = pl.multiple_of(i * 48, 16)
        for a in range(6):
            dst[pl.ds(at, 48), a * 128:(a + 1) * 128] = src[a, pl.ds(at, 48), :].astype(B)
        return 0
    lax.fori_loop(0, rows // 48, f, 0)


def big(w_ref, p_ref, k, o_ref):
    def f(i, _):
        at = pl.multiple_of(i * 432, 16)
        res = dot(w_ref[pl.ds(at, 432), :k], p_ref[:k, :])
        for a in range(6):
            o_ref[a, pl.ds(at, 432), :] = res[:, a * 128:(a + 1) * 128]
        return 0
    lax.fori_loop(0, 3, f, 0)
    o_ref[:, 1296:1440, :] = jnp.zeros((6, 144, 128), F)


def padded(x):
    return jnp.concatenate([x, jnp.zeros((x.shape[0], 32), F)], axis=1)


def clear_gaps(pf):
    for q in range(12):
        pf[:, q * 128 + 108:(q + 1) * 128, :] = jnp.zeros((6, 20, 128), F)


def compressed(x):
    return jnp.concatenate([x[:, g * 40:g * 40 + 36] for g in range(6)], axis=1)


def upper_kernel(order_ref, *refs):
    bufs = refs[:8]
    small_ref, wtop_hbm, wright_hbm, out_ref, ct_ref, tef, pf, p1, p3, o1, o3, tps, wtop_ref, wright_ref, sems = refs[8:]
    copies = load([(wtop_hbm, wtop_ref), (wright_hbm, wright_ref)], sems)
    expand(order_ref, bufs, 0, tef)
    uc = small_ref[648:744, :]
    rc = small_ref[744:840, :]
    tps[0:216, :] = small_ref[1024:1240, :].astype(F)
    tps[216:320, :] = jnp.zeros((104, 128), F)
    lu = dot(bufs[0][216:432, :][:, :96], uc).astype(B)[:, :96]
    ar = dot(small_ref[216:432, :], rc, NT).astype(B)
    for v in range(36):
        te = tef[pl.ds(v, 96, stride=36), :].astype(B)
        d1 = dot(lu, te)
        for a in range(6):
            pf[a, v * 36:(v + 1) * 36, :] = d1[a * 36:(a + 1) * 36, :]
    to_bf16(pf, p1, 1296)
    clear_gaps(pf)
    for v in range(36):
        te = tef[pl.ds(v, 96, stride=36), :].astype(B)
        d3 = padded(dot(ar, te[:, :96], NT))
        at = (v // 3) * 128 + (v % 3) * 36
        for a in range(6):
            pf[a, at:at + 36, :] = d3[a * 36:(a + 1) * 36, :]
    to_bf16(pf, p3, 1536)
    copies[0].wait()
    big(wtop_ref, p1, 1296, o1)
    copies[1].wait()
    big(wright_ref, p3, 1536, o3)
    acc = jnp.zeros((240, 256), F)
    for tp in range(18):
        xs = []
        ys = []
        for t in (2 * tp, 2 * tp + 1):
            xs.append(jnp.concatenate([o1[a, pl.ds(t, 40, stride=36), :] for a in range(6)], axis=0).astype(B))
            ys.append(jnp.concatenate([o3[g, pl.ds(t, 40, stride=36), :] for g in range(6)]
                                      + [tps[pl.ds(t, 8, stride=36), :], jnp.zeros((8, 128), F)], axis=0).astype(B))
        acc = acc + dot(jnp.concatenate(xs, axis=1), jnp.concatenate(ys, axis=1), NT)
    up = compressed(acc[:, :240] * jnp.float32(WIDE ** -0.5))
    for a in range(6):
        out_ref[a * 36:(a + 1) * 36, :] = up[a * 40:a * 40 + 36, :].astype(B)
    ct = jnp.transpose(acc[:, 128:256])[112:120, :]
    ct_ref[...] = compressed(ct)[0:6, :].astype(B)


def left_kernel(order_ref, *refs):
    bufs = refs[:8]
    small_ref, ber_ref, wtop_hbm, wbot_hbm, bpr_ref, out_ref, cb_ref, lef, pf, p2, p4, o2, o4, cbs, abf, wtop_ref, wbot_ref, sems = refs[8:]
    copies = load([(wtop_hbm, wtop_ref), (wbot_hbm, wbot_ref)], sems)
    expand(order_ref, bufs, 216, lef)
    uc = small_ref[648:744, :]
    lc = small_ref[840:936, :]
    at = dot(small_ref[0:216, :], uc, NT).astype(B)
    abf[0:216, :] = padded(dot(ber_ref[...], lc, NT))
    ab = jnp.concatenate([abf[pl.ds(b * 36 + h, 12, stride=3), :] for b in range(6) for h in range(3)], axis=0).astype(B)[:, :96]
    for u in range(36):
        le = lef[pl.ds(u, 96, stride=36), :].astype(B)
        d2 = padded(dot(at, le[:, :96], NT))
        for b in range(6):
            pf[b, pl.ds(u, 36, stride=36), :] = d2[b * 36:(b + 1) * 36, :]
    to_bf16(pf, p2, 1296)
    clear_gaps(pf)
    for u in range(36):
        le = lef[pl.ds(u, 96, stride=36), :].astype(B)
        d4 = dot(ab, le)
        for b in range(6):
            for h in range(3):
                pf[b, pl.ds(h * 36 + u, 12, stride=128), :] = d4[b * 36 + h * 12:b * 36 + h * 12 + 12, :]
    to_bf16(pf, p4, 1536)
    copies[0].wait()
    big(wtop_ref, p2, 1296, o2)
    copies[1].wait()
    big(wbot_ref, p4, 1536, o4)
    acc = jnp.zeros((240, 240), F)
    for sp in range(18):
        xs = []
        ys = []
        for s in (2 * sp, 2 * sp + 1):
            x = jnp.concatenate([o2[b, s * 36:s * 36 + 40, :] for b in range(6)], axis=0).astype(B)
            y = jnp.concatenate([o4[b, s * 36:s * 36 + 40, :] for b in range(6)], axis=0).astype(B)
            xs.append(x)
            ys.append(y)
            cbs[pl.ds(s, 8, stride=36), :] = dot(bpr_ref[...], y)
        acc = acc + dot(jnp.concatenate(xs, axis=1), jnp.concatenate(ys, axis=1), NT)
    lh = compressed(acc * jnp.float32(WIDE ** -0.5))
    for a in range(6):
        out_ref[a * 36:(a + 1) * 36, :] = lh[a * 40:a * 40 + 36, :].astype(B)
    sums = jnp.transpose(cbs[0:256, :])
    cb_ref[...] = jnp.zeros((128, 256), F)
    for m in range(16):
        at = ((m % 4) * 4 + ((m // 4) % 2) * 2 + m // 8) * 6
        cb_ref[8 * m:8 * m + 6, :] = sums[at:at + 6, :]


def scratch():
    return [pltpu.VMEM((WIDE, 128), F), pltpu.VMEM((6, 2048, 128), F), pltpu.VMEM((1536, 768), B),
            pltpu.VMEM((1536, 768), B), pltpu.VMEM((6, 1440, 128), F), pltpu.VMEM((6, 1440, 128), F)]


def prepare(*args):
    return pl.pallas_call(
        prepare_kernel, out_shape=(shape_of(16, 216), shape_of(64, 128), shape_of(200, 216)),
        in_specs=[HB] * 9, out_specs=(VM,) * 3,
        scratch_shapes=[pltpu.VMEM(x.shape, B) for x in args] + [pltpu.SemaphoreType.DMA((9,))],
        name="prepare")(*args)


def pieces(at, turned, piece):
    return pl.pallas_call(pieces_kernel, out_shape=(shape_of(24, 216), shape_of(16, 128), shape_of(8, 240)),
                          in_specs=[SM, VM, VM], out_specs=(VM,) * 3, name="pieces",
                          compiler_params=params(4))(at, turned, piece)


def form_copies():
    return [pltpu.VMEM((1296, 1408), B), pltpu.VMEM((1296, 1536), B), pltpu.SemaphoreType.DMA((2,))]


def upper(order, bufs, small, wtop, wright):
    return pl.pallas_call(
        upper_kernel, out_shape=(shape_of(216, 216), shape_of(6, 216)), in_specs=[SM] + [VM] * 9 + [HB] * 2,
        out_specs=(VM, VM), scratch_shapes=scratch() + [pltpu.VMEM((320, 128), F)] + form_copies(), name="upper",
        compiler_params=params(50), cost_estimate=work(8 << 30))(order, *bufs, small, wtop, wright)


def left(order, bufs, small, ber, wtop, wbot, bpr):
    return pl.pallas_call(
        left_kernel, out_shape=(shape_of(216, 216), shape_of(128, 256, kind=F)),
        in_specs=[SM] + [VM] * 10 + [HB] * 2 + [VM], out_specs=(VM, VM),
        scratch_shapes=scratch() + [pltpu.VMEM((288, 128), F), pltpu.VMEM((232, 128), F)] + form_copies(), name="left",
        compiler_params=params(50), cost_estimate=work(8 << 30))(order, *bufs, small, ber, wtop, wbot, bpr)


def finish_kernel(own, one, two, three, out_ref):
    res = own[...] + one[...] + two[...] + three[...]
    rows = [jnp.concatenate([res[a:a + 1, x * 36:(x + 1) * 36] for a in range(6)], axis=1) for x in range(6)]
    out_ref[...] = jnp.concatenate(rows, axis=0).astype(B)


def finish(*parts):
    return pl.pallas_call(finish_kernel, out_shape=shape_of(6, 216), in_specs=[VM] * 4, out_specs=VM,
                          name="finish", compiler_params=params(4))(*parts)


def lanes_shifted(a_ref, z_ref, pair):
    tile = (pair * 72) // 128
    base = pl.multiple_of(tile * 128, 128)
    off = pair * 72 - tile * 128
    k = lax.broadcasted_iota(jnp.int32, (256, 256), 0)
    n = lax.broadcasted_iota(jnp.int32, (256, 256), 1)
    w = n % 128
    sel = ((k == off + (n // 128) * 36 + w % 36) & (w < 108)).astype(B)
    z_ref[...] = dot(a_ref[:, pl.ds(base, 256)], sel)


def realign(a_ref, z_ref, o_ref, out_hbm, sem):
    lane = lax.broadcasted_iota(jnp.int32, (36, 128), 1)

    def f(g, _):
        strips = []
        for h in range(2):
            lanes_shifted(a_ref, z_ref.at[h], 2 * g + h)
        for h in range(2):
            for q in range(2):
                tiles = []
                for m in range(12):
                    z = [z_ref[h, (3 * m + e) * 36:(3 * m + e + 1) * 36, q * 128:(q + 1) * 128] for e in range(3)]
                    tiles.append(jnp.where(lane < 36, z[0], jnp.where(lane < 72, z[1], z[2])))
                strips.append(jnp.concatenate(tiles, axis=1))
        at = pl.multiple_of(g * 144, 16)
        o_ref[pl.ds(at, 144), :] = jnp.concatenate(strips, axis=0).astype(B)
        pltpu.make_async_copy(o_ref.at[pl.ds(at, 144), :], out_hbm.at[pl.ds(at, 144), :], sem.at[g]).start()
        return 0
    lax.fori_loop(0, 9, f, 0)

    def w(g, _):
        at = pl.multiple_of(g * 144, 16)
        pltpu.make_async_copy(o_ref.at[pl.ds(at, 144), :], out_hbm.at[pl.ds(at, 144), :], sem.at[g]).wait()
        return 0
    lax.fori_loop(0, 9, w, 0)


def right_form_kernel(s_hbm, wright_hbm, apad, z, o, sems, done):
    load([(s_hbm, apad)], sems)[0].wait()
    realign(apad, z, o, wright_hbm, done)


def left_forms_kernel(s_hbm, wtop_hbm, wbot_hbm, apad, z, o, sems, done, s_ref):
    load([(s_hbm, s_ref)], sems)[0].wait()
    eye = (lax.broadcasted_iota(jnp.int32, (128, 128), 0) == lax.broadcasted_iota(jnp.int32, (128, 128), 1)).astype(B)
    for b in range(11):
        n = min(128, 1296 - b * 128)
        apad[b * 128:b * 128 + n, :1296] = dot(eye[:n, :n], s_ref[:, b * 128:b * 128 + n], NT).astype(B)
    apad[:, 1296:1408] = jnp.zeros((1296, 112), B)
    out = pltpu.make_async_copy(apad, wtop_hbm, sems.at[0])
    out.start()
    realign(apad, z, o, wbot_hbm, done)
    out.wait()


def flat_form_kernel(x_ref, s_hbm, wide, tiles, s_ref, sems):
    def widen(i, _):
        at = pl.multiple_of(i * 256, 16)
        wide[pl.ds(at, 256), :] = x_ref[pl.ds(at, 256), :].astype(F)
        return 0
    lax.fori_loop(0, 51, widen, 0)
    wide[13056:13122, :] = x_ref[13056:13122, :].astype(F)
    lane = lax.broadcasted_iota(jnp.int32, (162, 128), 1)
    for i in range(8):
        def turn(j):
            v = wide[pl.ds(10 * i + j, 162, stride=81), :]
            return pltpu.roll(v, 128 - 16 * i, 1) if i else v
        here = turn(0)
        for j in range(11):
            if j == 10:
                tile = jnp.where(lane < 16, here, 0.0)
            else:
                after = turn(j + 1)
                tile = jnp.where(lane < 128 - 16 * i, here, after) if i else here
                here = after
            tiles[j, pl.ds(i, 162, stride=8), :] = tile

    def narrow(g, _):
        at = pl.multiple_of(g * 144, 16)
        for j in range(11):
            s_ref[pl.ds(at, 144), 128 * j:128 * j + 128] = tiles[j, pl.ds(at, 144), :].astype(B)
        pltpu.make_async_copy(s_ref.at[pl.ds(at, 144), :], s_hbm.at[pl.ds(at, 144), :], sems.at[g]).start()
        return 0
    lax.fori_loop(0, 9, narrow, 0)

    def w(g, _):
        at = pl.multiple_of(g * 144, 16)
        pltpu.make_async_copy(s_ref.at[pl.ds(at, 144), :], s_hbm.at[pl.ds(at, 144), :], sems.at[g]).wait()
        return 0
    lax.fori_loop(0, 9, w, 0)


def form_scratch():
    return [pltpu.VMEM((1296, 1408), B), pltpu.VMEM((2, 1296, 256), F), pltpu.VMEM((1296, 1536), B),
            pltpu.SemaphoreType.DMA((1,)), pltpu.SemaphoreType.DMA((9,))]


def flat_form(flat):
    return pl.pallas_call(flat_form_kernel, out_shape=shape_of(1296, 1408), in_specs=[VM], out_specs=HB,
                          scratch_shapes=[pltpu.VMEM((13616, 128), F), pltpu.VMEM((11, 1344, 128), F),
                                          pltpu.VMEM((1296, 1408), B), pltpu.SemaphoreType.DMA((9,))],
                          name="flat_form", compiler_params=params(60), cost_estimate=work(3 << 30))(flat)


def right_form(s2):
    return pl.pallas_call(right_form_kernel, out_shape=shape_of(1296, 1536), in_specs=[HB], out_specs=HB,
                          scratch_shapes=form_scratch(), name="right_form", compiler_params=params(60),
                          cost_estimate=work(3 << 30))(s2)


def left_forms(s2):
    return pl.pallas_call(left_forms_kernel, out_shape=(shape_of(1296, 1408), shape_of(1296, 1536)), in_specs=[HB],
                          out_specs=(HB, HB), scratch_shapes=form_scratch() + [pltpu.VMEM((1296, 1408), B)],
                          name="left_forms", compiler_params=params(60), cost_estimate=work(4 << 30))(s2)


ROW, COL = "row", "col"


def row_permute(x, move):
    pairs = []
    for y in range(4):
        for z in range(2):
            for k in range(2):
                a, b, c = move(y, z, k)
                pairs.append((y * 4 + z * 2 + k, a * 4 + b * 2 + c))
    return lax.ppermute(x, ROW, pairs)


def col_permute(x, move):
    pairs = []
    for z in range(4):
        for i in range(4):
            a, b = move(z, i)
            pairs.append((z * 4 + i, a * 4 + b))
    return lax.ppermute(x, COL, pairs)


def swap_axes(x):
    pairs = [(r * 16 + c, c * 16 + r) for r in range(16) for c in range(16)]
    return lax.ppermute(x, (ROW, COL), pairs)


def stacked(own, received):
    return jnp.concatenate([own, *received], axis=0)


def other_core(x):
    return row_permute(x, lambda a, b, k: (a, b, 1 - k))


def other_z(x):
    return row_permute(x, lambda a, b, k: (a, 1 - b, k))


def along_y(x, s):
    return row_permute(x, lambda a, b, k: ((a + s) % 4, b, k))


def shards(uc, rc, lc, te, re, be, le, site_flat, tp, bp):
    r = lax.axis_index(ROW)
    c = lax.axis_index(COL)
    y, zlo, core = r // 4, (r // 2) % 2, r % 2
    zhi, x = c // 4, c % 4
    hold = lax.optimization_barrier

    piece, pack, turned = prepare(te, re, be, le, uc.T, rc.T, lc.T, tp.T, bp.T)
    swapped = swap_axes(turned)
    s2 = flat_form(hold((site_flat, turned))[0].reshape(13122, 128))
    swapped, s2 = hold((swapped, s2))
    piece, tpx, bpr = pieces((c * 6).astype(jnp.int32).reshape(1), swapped, piece)

    piece = stacked(piece, [col_permute(piece, lambda z, i, s=s: ((z + s) % 4, i)) for s in (1, 2, 3)])
    piece = stacked(piece, [col_permute(piece, lambda z, i, s=s: (z, (i + s) % 4)) for s in (1, 2, 3)])
    at = jnp.arange(384)
    x_rel, z_rel, edge, j = at // 96, (at // 24) % 4, (at // 8) % 3, at % 8
    block = ((zhi - z_rel) % 4) * 4 + (x - x_rel) % 4
    target = jnp.where(j < 6, edge * 128 + block * 6 + j, -1)
    place = (target[:, None] == at[None, :]).astype(B)
    rows = lax.dot_general(piece, place, (((0,), (0,)), ((), ())), preferred_element_type=F).astype(B)
    ber = rows[:, 256:]

    own = jnp.concatenate([rows[:, :128], rows[:, 128:256], pack, tpx], axis=0)
    near = stacked(own, [other_z(own)])
    far = [along_y(near, s) for s in (1, 2, 3)]
    near_twin = other_core(near)
    wtop, wbot = left_forms(hold((s2, near))[0])
    *far, near_twin, wtop = hold((*far, near_twin, wtop))
    far_twin = [other_core(f) for f in far]
    bufs = [near, *far, near_twin, *far_twin]
    rel = jnp.arange(16)
    order = ((y - (rel // 2) % 4) % 4) * 4 + (zlo ^ (rel % 2)) * 2 + (core ^ (rel // 8))
    order = order.astype(jnp.int32)

    small = gather_small(order, bufs)

    lf, cb = left(order, bufs, small, ber, wtop, wbot, bpr)
    part = lambda v, n, size: lax.dynamic_slice_in_dim(v, n * size, size, 0)
    cb = part(cb, core, 64) + other_core(part(cb, 1 - core, 64))
    cb_z = other_z(part(cb, 1 - zlo, 32))
    wright = right_form(hold((s2, cb))[0])
    cb_z, wright = hold((cb_z, wright))
    cb = part(cb, zlo, 32) + cb_z
    cb_y = [along_y(part(cb, (y + s) % 4, 8), s) for s in (1, 2, 3)]
    order = hold((order, cb))[0]
    up, corner_top = upper(order, bufs, small, wtop, wright)
    *cb_y, up = hold((*cb_y, up))
    corner_bottom = finish(part(cb, y, 8), *cb_y)
    return up, lf, corner_top, corner_bottom


def solution(mesh):
    placed = (
        P(None, ROW),
        P(None, ROW),
        P(None, ROW),
        P(ROW, COL, None),
        P(ROW, COL, None),
        P(ROW, COL, None),
        P(ROW, COL, None),
        P(),
        P(COL, None),
        P(COL, None),
    )
    return jax.shard_map(
        shards,
        mesh=mesh,
        in_specs=placed,
        out_specs=(P(ROW, COL), P(COL, ROW), P(COL, ROW), P(COL, ROW)),
        check_vma=False,
    )
```

```python
import jax
import jax.numpy as jnp
from jax import lax
from jax.experimental import pallas as pl
from jax.experimental.pallas import tpu as pltpu
from jax.sharding import PartitionSpec as P

F = jnp.float32
B = jnp.bfloat16
NN = (((1,), (0,)), ((), ()))
NT = (((1,), (1,)), ((), ()))
VM = pl.BlockSpec(memory_space=pltpu.VMEM)
SM = pl.BlockSpec(memory_space=pltpu.SMEM)
HB = pl.BlockSpec(memory_space=pltpu.HBM)
BLOCK = 512
WIDE = 3456


def dot(x, y, dims=NN):
    return lax.dot_general(x, y, dims, preferred_element_type=F)


def shape_of(*dims, kind=B):
    return jax.ShapeDtypeStruct(dims, kind)


def params(mib):
    return pltpu.CompilerParams(vmem_limit_bytes=mib << 20)


def work(flops):
    return pl.CostEstimate(flops=flops, transcendentals=0, bytes_accessed=1 << 22)


def load(pairs, sems):
    copies = [pltpu.make_async_copy(src, dst, sems.at[n]) for n, (src, dst) in enumerate(pairs)]
    for cp in copies:
        cp.start()
    return copies


def prepare_kernel(at_ref, *refs):
    hbm, (piece, pack, turned), local, sems = refs[:9], refs[9:12], refs[12:21], refs[21]
    for cp in load(list(zip(hbm, local)), sems):
        cp.wait()
    te, re, be, le, uct, rct, lct, tpt, bpt = local
    zero = jnp.zeros((2, 216), B)
    for n, e in ((0, te), (1, le)):
        v = e[...].astype(F)
        piece[8 * n:8 * n + 8, :] = jnp.concatenate(
            [jnp.concatenate([v[i] for i in range(6)], axis=1).astype(B), zero], axis=0)
    parts = []
    for e in (te, re, be):
        v = e[...].astype(F)
        parts.append(jnp.concatenate([v[:, j, :] for j in range(6)], axis=1))
    row = lax.broadcasted_iota(jnp.int32, (8, 96), 0)
    lane = lax.broadcasted_iota(jnp.int32, (8, 96), 1)
    pick = ((lane == at_ref[0] + row) & (row < 6)).astype(B)
    turned[0:8, :] = dot(pick, tpt[...]).astype(B)
    turned[8:16, :] = dot(pick, bpt[...]).astype(B)
    turned[16:24, :] = jnp.concatenate([parts[2].astype(B), zero], axis=0)
    for c in (uct, rct, lct):
        parts.append(c[...].astype(F))
    flat = jnp.concatenate(parts + [jnp.zeros((6, 88), F)], axis=1)
    flat = jnp.concatenate([flat, jnp.zeros((2, 1024), F)], axis=0).astype(B)
    for k in range(8):
        pack[8 * k:8 * k + 8, :] = flat[:, 128 * k:128 * k + 128]


def pieces_kernel(turned, piece, out, tpx, bpr):
    out[0:16, :] = piece[...]
    out[16:24, :] = turned[16:24, :]
    top = turned[0:8, :].astype(F)
    flat = jnp.concatenate(
        [jnp.concatenate([top[x:x + 1, b * 36:(b + 1) * 36] for x in range(6)], axis=1) for b in range(6)], axis=0)
    flat = jnp.concatenate([flat, jnp.zeros((6, 40), F)], axis=1)
    flat = jnp.concatenate([flat, jnp.zeros((2, 256), F)], axis=0).astype(B)
    tpx[0:8, :] = flat[:, :128]
    tpx[8:16, :] = flat[:, 128:]
    bottom = turned[8:16, :].astype(F)
    gap = jnp.zeros((8, 4), F)
    bpr[...] = jnp.concatenate([y for b in range(6) for y in (bottom[:, b * 36:(b + 1) * 36], gap)], axis=1).astype(B)


def expand(order_ref, bufs, off, dst):
    for rel in range(16):
        at = pl.multiple_of(order_ref[rel] * 216, 8)
        start = (rel % 2) * BLOCK + off
        dst[pl.ds(at, 216), :] = bufs[rel // 2][start:start + 216, :].astype(F)


def gather_small_kernel(order_ref, *refs):
    bufs = refs[:8]
    out_ref, packs = refs[8:]
    for rel in range(16):
        at = pl.multiple_of(order_ref[rel] * 8, 8)
        start = (rel % 2) * BLOCK + 432
        for k in range(10):
            packs[k, pl.ds(at, 8), :] = bufs[rel // 2][start + 8 * k:start + 8 * k + 8, :].astype(F)
    row = lax.broadcasted_iota(jnp.int32, (128, 128), 0)
    lane = lax.broadcasted_iota(jnp.int32, (128, 128), 1)
    place = ((row % 8 < 6) & (lane == (row // 8) * 6 + row % 8)).astype(B)
    for k in range(10):
        out_ref[k * 128:(k + 1) * 128, :] = dot(jnp.transpose(packs[k]).astype(B), place).astype(B)


def gather_small(order, bufs):
    return pl.pallas_call(gather_small_kernel, out_shape=shape_of(1280, 128), in_specs=[SM] + [VM] * 8, out_specs=VM,
                          scratch_shapes=[pltpu.VMEM((10, 128, 128), F)], name="gather_small",
                          compiler_params=params(6))(order, *bufs)


def to_bf16(src, dst, rows):
    def f(i, _):
        at = pl.multiple_of(i * 48, 16)
        for a in range(6):
            dst[pl.ds(at, 48), a * 128:(a + 1) * 128] = src[a, pl.ds(at, 48), :].astype(B)
        return 0
    lax.fori_loop(0, rows // 48, f, 0)


def big(w_ref, p_ref, k, o_ref):
    def f(i, _):
        at = pl.multiple_of(i * 432, 16)
        res = dot(w_ref[pl.ds(at, 432), :k], p_ref[:k, :])
        for a in range(6):
            o_ref[a, pl.ds(at, 432), :] = res[:, a * 128:(a + 1) * 128]
        return 0
    lax.fori_loop(0, 3, f, 0)
    o_ref[:, 1296:1440, :] = jnp.zeros((6, 144, 128), F)


def padded(x):
    return jnp.concatenate([x, jnp.zeros((x.shape[0], 32), F)], axis=1)


def clear_gaps(pf):
    for q in range(12):
        pf[:, q * 128 + 108:(q + 1) * 128, :] = jnp.zeros((6, 20, 128), F)


def compressed(x):
    return jnp.concatenate([x[:, g * 40:g * 40 + 36] for g in range(6)], axis=1)


def upper_kernel(order_ref, *refs):
    bufs = refs[:8]
    small_ref, wtop_hbm, wright_hbm, out_ref, ct_ref, tef, pf, p1, p3, o1, o3, tps, wtop_ref, wright_ref, sems = refs[8:]
    copies = load([(wtop_hbm, wtop_ref), (wright_hbm, wright_ref)], sems)
    expand(order_ref, bufs, 0, tef)
    uc = small_ref[648:744, :]
    rc = small_ref[744:840, :]
    tps[0:216, :] = small_ref[1024:1240, :].astype(F)
    tps[216:320, :] = jnp.zeros((104, 128), F)
    lu = dot(bufs[0][216:432, :][:, :96], uc).astype(B)[:, :96]
    ar = dot(small_ref[216:432, :], rc, NT).astype(B)
    for v in range(36):
        te = tef[pl.ds(v, 96, stride=36), :].astype(B)
        d1 = dot(lu, te)
        for a in range(6):
            pf[a, v * 36:(v + 1) * 36, :] = d1[a * 36:(a + 1) * 36, :]
    to_bf16(pf, p1, 1296)
    clear_gaps(pf)
    for v in range(36):
        te = tef[pl.ds(v, 96, stride=36), :].astype(B)
        d3 = padded(dot(ar, te[:, :96], NT))
        at = (v // 3) * 128 + (v % 3) * 36
        for a in range(6):
            pf[a, at:at + 36, :] = d3[a * 36:(a + 1) * 36, :]
    to_bf16(pf, p3, 1536)
    copies[0].wait()
    big(wtop_ref, p1, 1296, o1)
    copies[1].wait()
    big(wright_ref, p3, 1536, o3)
    acc = jnp.zeros((240, 256), F)
    for tp in range(18):
        xs = []
        ys = []
        for t in (2 * tp, 2 * tp + 1):
            xs.append(jnp.concatenate([o1[a, pl.ds(t, 40, stride=36), :] for a in range(6)], axis=0).astype(B))
            ys.append(jnp.concatenate([o3[g, pl.ds(t, 40, stride=36), :] for g in range(6)]
                                      + [tps[pl.ds(t, 8, stride=36), :], jnp.zeros((8, 128), F)], axis=0).astype(B))
        acc = acc + dot(jnp.concatenate(xs, axis=1), jnp.concatenate(ys, axis=1), NT)
    up = compressed(acc[:, :240] * jnp.float32(WIDE ** -0.5))
    for a in range(6):
        out_ref[a * 36:(a + 1) * 36, :] = up[a * 40:a * 40 + 36, :].astype(B)
    ct = jnp.transpose(acc[:, 128:256])[112:120, :]
    ct_ref[...] = compressed(ct)[0:6, :].astype(B)


def left_kernel(order_ref, *refs):
    bufs = refs[:8]
    small_ref, ber_ref, wtop_hbm, wbot_hbm, bpr_ref, out_ref, cb_ref, lef, pf, p2, p4, o2, o4, cbs, abf, wtop_ref, wbot_ref, sems = refs[8:]
    copies = load([(wtop_hbm, wtop_ref), (wbot_hbm, wbot_ref)], sems)
    expand(order_ref, bufs, 216, lef)
    uc = small_ref[648:744, :]
    lc = small_ref[840:936, :]
    at = dot(small_ref[0:216, :], uc, NT).astype(B)
    abf[0:216, :] = padded(dot(ber_ref[...], lc, NT))
    ab = jnp.concatenate([abf[pl.ds(b * 36 + h, 12, stride=3), :] for b in range(6) for h in range(3)], axis=0).astype(B)[:, :96]
    for u in range(36):
        le = lef[pl.ds(u, 96, stride=36), :].astype(B)
        d2 = padded(dot(at, le[:, :96], NT))
        for b in range(6):
            pf[b, pl.ds(u, 36, stride=36), :] = d2[b * 36:(b + 1) * 36, :]
    to_bf16(pf, p2, 1296)
    clear_gaps(pf)
    for u in range(36):
        le = lef[pl.ds(u, 96, stride=36), :].astype(B)
        d4 = dot(ab, le)
        for b in range(6):
            for h in range(3):
                pf[b, pl.ds(h * 36 + u, 12, stride=128), :] = d4[b * 36 + h * 12:b * 36 + h * 12 + 12, :]
    to_bf16(pf, p4, 1536)
    copies[0].wait()
    big(wtop_ref, p2, 1296, o2)
    copies[1].wait()
    big(wbot_ref, p4, 1536, o4)
    acc = jnp.zeros((240, 240), F)
    for sp in range(18):
        xs = []
        ys = []
        for s in (2 * sp, 2 * sp + 1):
            x = jnp.concatenate([o2[b, s * 36:s * 36 + 40, :] for b in range(6)], axis=0).astype(B)
            y = jnp.concatenate([o4[b, s * 36:s * 36 + 40, :] for b in range(6)], axis=0).astype(B)
            xs.append(x)
            ys.append(y)
            cbs[pl.ds(s, 8, stride=36), :] = dot(bpr_ref[...], y)
        acc = acc + dot(jnp.concatenate(xs, axis=1), jnp.concatenate(ys, axis=1), NT)
    lh = compressed(acc * jnp.float32(WIDE ** -0.5))
    for a in range(6):
        out_ref[a * 36:(a + 1) * 36, :] = lh[a * 40:a * 40 + 36, :].astype(B)
    sums = jnp.transpose(cbs[0:256, :])
    cb_ref[...] = jnp.zeros((128, 256), F)
    for m in range(16):
        at = ((m % 4) * 4 + ((m // 4) % 2) * 2 + m // 8) * 6
        cb_ref[8 * m:8 * m + 6, :] = sums[at:at + 6, :]


def scratch():
    return [pltpu.VMEM((WIDE, 128), F), pltpu.VMEM((6, 2048, 128), F), pltpu.VMEM((1536, 768), B),
            pltpu.VMEM((1536, 768), B), pltpu.VMEM((6, 1440, 128), F), pltpu.VMEM((6, 1440, 128), F)]


def prepare(at, *args):
    return pl.pallas_call(
        prepare_kernel, out_shape=(shape_of(16, 216), shape_of(64, 128), shape_of(24, 216)),
        in_specs=[SM] + [HB] * 9, out_specs=(VM,) * 3,
        scratch_shapes=[pltpu.VMEM(x.shape, B) for x in args] + [pltpu.SemaphoreType.DMA((9,))],
        name="prepare")(at, *args)


def pieces(turned, piece):
    return pl.pallas_call(pieces_kernel, out_shape=(shape_of(24, 216), shape_of(16, 128), shape_of(8, 240)),
                          in_specs=[VM, VM], out_specs=(VM,) * 3, name="pieces",
                          compiler_params=params(4))(turned, piece)


def form_copies():
    return [pltpu.VMEM((1296, 1408), B), pltpu.VMEM((1296, 1536), B), pltpu.SemaphoreType.DMA((2,))]


def upper(order, bufs, small, wtop, wright):
    return pl.pallas_call(
        upper_kernel, out_shape=(shape_of(216, 216), shape_of(6, 216)), in_specs=[SM] + [VM] * 9 + [HB] * 2,
        out_specs=(VM, VM), scratch_shapes=scratch() + [pltpu.VMEM((320, 128), F)] + form_copies(), name="upper",
        compiler_params=params(50), cost_estimate=work(8 << 30))(order, *bufs, small, wtop, wright)


def left(order, bufs, small, ber, wtop, wbot, bpr):
    return pl.pallas_call(
        left_kernel, out_shape=(shape_of(216, 216), shape_of(128, 256, kind=F)),
        in_specs=[SM] + [VM] * 10 + [HB] * 2 + [VM], out_specs=(VM, VM),
        scratch_shapes=scratch() + [pltpu.VMEM((288, 128), F), pltpu.VMEM((232, 128), F)] + form_copies(), name="left",
        compiler_params=params(50), cost_estimate=work(8 << 30))(order, *bufs, small, ber, wtop, wbot, bpr)


def finish_kernel(own, one, two, three, out_ref):
    res = own[...] + one[...] + two[...] + three[...]
    rows = [jnp.concatenate([res[a:a + 1, x * 36:(x + 1) * 36] for a in range(6)], axis=1) for x in range(6)]
    out_ref[...] = jnp.concatenate(rows, axis=0).astype(B)


def finish(*parts):
    return pl.pallas_call(finish_kernel, out_shape=shape_of(6, 216), in_specs=[VM] * 4, out_specs=VM,
                          name="finish", compiler_params=params(4))(*parts)


def lanes_shifted(a_ref, z_ref, pair):
    tile = (pair * 72) // 128
    base = pl.multiple_of(tile * 128, 128)
    off = pair * 72 - tile * 128
    k = lax.broadcasted_iota(jnp.int32, (256, 256), 0)
    n = lax.broadcasted_iota(jnp.int32, (256, 256), 1)
    w = n % 128
    sel = ((k == off + (n // 128) * 36 + w % 36) & (w < 108)).astype(B)
    z_ref[...] = dot(a_ref[:, pl.ds(base, 256)], sel)


def column_chunks(src, dst, sems):
    ends = (0, 384, 768, 1152, 1408)
    return load([(src.at[:, p:q], dst.at[:, p:q]) for p, q in zip(ends, ends[1:])], sems)


def realign(a_ref, z_ref, o_ref, out_hbm, sem, chunks=()):
    lane = lax.broadcasted_iota(jnp.int32, (36, 128), 1)

    def f(g, _):
        for n, cp in zip((0, 2, 4, 7), chunks):
            @pl.when(g == n)
            def _(cp=cp):
                cp.wait()
        strips = []
        for h in range(2):
            lanes_shifted(a_ref, z_ref.at[h], 2 * g + h)
        for h in range(2):
            for q in range(2):
                tiles = []
                for m in range(12):
                    z = [z_ref[h, (3 * m + e) * 36:(3 * m + e + 1) * 36, q * 128:(q + 1) * 128] for e in range(3)]
                    tiles.append(jnp.where(lane < 36, z[0], jnp.where(lane < 72, z[1], z[2])))
                strips.append(jnp.concatenate(tiles, axis=1))
        at = pl.multiple_of(g * 144, 16)
        o_ref[pl.ds(at, 144), :] = jnp.concatenate(strips, axis=0).astype(B)
        pltpu.make_async_copy(o_ref.at[pl.ds(at, 144), :], out_hbm.at[pl.ds(at, 144), :], sem.at[g]).start()
        return 0
    lax.fori_loop(0, 9, f, 0)

    def w(g, _):
        at = pl.multiple_of(g * 144, 16)
        pltpu.make_async_copy(o_ref.at[pl.ds(at, 144), :], out_hbm.at[pl.ds(at, 144), :], sem.at[g]).wait()
        return 0
    lax.fori_loop(0, 9, w, 0)


def right_form_kernel(s_hbm, wright_hbm, apad, z, o, sems, done):
    realign(apad, z, o, wright_hbm, done, column_chunks(s_hbm, apad, sems))


def left_forms_kernel(s_hbm, wtop_hbm, wbot_hbm, apad, z, o, sems, done, s_ref):
    chunks = column_chunks(s_hbm, s_ref, sems)
    eye = (lax.broadcasted_iota(jnp.int32, (128, 128), 0) == lax.broadcasted_iota(jnp.int32, (128, 128), 1)).astype(B)
    for b in range(11):
        n = min(128, 1296 - b * 128)
        if b % 3 == 0:
            chunks[b // 3].wait()
        apad[b * 128:b * 128 + n, :1296] = dot(eye[:n, :n], s_ref[:, b * 128:b * 128 + n], NT).astype(B)
    apad[:, 1296:1408] = jnp.zeros((1296, 112), B)
    out = pltpu.make_async_copy(apad, wtop_hbm, sems.at[0])
    out.start()
    realign(apad, z, o, wbot_hbm, done)
    out.wait()


def flat_form_kernel(x_ref, s_hbm, wide, tiles, s_ref, sems):
    def widen(i, _):
        at = pl.multiple_of(i * 256, 16)
        wide[pl.ds(at, 256), :] = x_ref[pl.ds(at, 256), :].astype(F)
        return 0
    lax.fori_loop(0, 51, widen, 0)
    wide[13056:13122, :] = x_ref[13056:13122, :].astype(F)
    lane = lax.broadcasted_iota(jnp.int32, (162, 128), 1)
    for i in range(8):
        def turn(j):
            v = wide[pl.ds(10 * i + j, 162, stride=81), :]
            return pltpu.roll(v, 128 - 16 * i, 1) if i else v
        here = turn(0)
        for j in range(11):
            if j == 10:
                tile = jnp.where(lane < 16, here, 0.0)
            else:
                after = turn(j + 1)
                tile = jnp.where(lane < 128 - 16 * i, here, after) if i else here
                here = after
            tiles[j, pl.ds(i, 162, stride=8), :] = tile

    def narrow(g, _):
        at = pl.multiple_of(g * 144, 16)
        for j in range(11):
            s_ref[pl.ds(at, 144), 128 * j:128 * j + 128] = tiles[j, pl.ds(at, 144), :].astype(B)
        pltpu.make_async_copy(s_ref.at[pl.ds(at, 144), :], s_hbm.at[pl.ds(at, 144), :], sems.at[g]).start()
        return 0
    lax.fori_loop(0, 9, narrow, 0)

    def w(g, _):
        at = pl.multiple_of(g * 144, 16)
        pltpu.make_async_copy(s_ref.at[pl.ds(at, 144), :], s_hbm.at[pl.ds(at, 144), :], sems.at[g]).wait()
        return 0
    lax.fori_loop(0, 9, w, 0)


def form_scratch():
    return [pltpu.VMEM((1296, 1408), B), pltpu.VMEM((2, 1296, 256), F), pltpu.VMEM((1296, 1536), B),
            pltpu.SemaphoreType.DMA((4,)), pltpu.SemaphoreType.DMA((9,))]


def flat_form(flat):
    return pl.pallas_call(flat_form_kernel, out_shape=shape_of(1296, 1408), in_specs=[VM], out_specs=HB,
                          scratch_shapes=[pltpu.VMEM((13616, 128), F), pltpu.VMEM((11, 1344, 128), F),
                                          pltpu.VMEM((1296, 1408), B), pltpu.SemaphoreType.DMA((9,))],
                          name="flat_form", compiler_params=params(60), cost_estimate=work(3 << 30))(flat)


def right_form(s2):
    return pl.pallas_call(right_form_kernel, out_shape=shape_of(1296, 1536), in_specs=[HB], out_specs=HB,
                          scratch_shapes=form_scratch(), name="right_form", compiler_params=params(60),
                          cost_estimate=work(3 << 30))(s2)


def left_forms(s2):
    return pl.pallas_call(left_forms_kernel, out_shape=(shape_of(1296, 1408), shape_of(1296, 1536)), in_specs=[HB],
                          out_specs=(HB, HB), scratch_shapes=form_scratch() + [pltpu.VMEM((1296, 1408), B)],
                          name="left_forms", compiler_params=params(60), cost_estimate=work(4 << 30))(s2)


ROW, COL = "row", "col"


def row_permute(x, move):
    pairs = []
    for y in range(4):
        for z in range(2):
            for k in range(2):
                a, b, c = move(y, z, k)
                pairs.append((y * 4 + z * 2 + k, a * 4 + b * 2 + c))
    return lax.ppermute(x, ROW, pairs)


def col_permute(x, move):
    pairs = []
    for z in range(4):
        for i in range(4):
            a, b = move(z, i)
            pairs.append((z * 4 + i, a * 4 + b))
    return lax.ppermute(x, COL, pairs)


def swap_axes(x):
    pairs = [(r * 16 + c, c * 16 + r) for r in range(16) for c in range(16)]
    return lax.ppermute(x, (ROW, COL), pairs)


def stacked(own, received):
    return jnp.concatenate([own, *received], axis=0)


def other_core(x):
    return row_permute(x, lambda a, b, k: (a, b, 1 - k))


def other_z(x):
    return row_permute(x, lambda a, b, k: (a, 1 - b, k))


def along_y(x, s):
    return row_permute(x, lambda a, b, k: ((a + s) % 4, b, k))


def shards(uc, rc, lc, te, re, be, le, site_flat, tp, bp):
    r = lax.axis_index(ROW)
    c = lax.axis_index(COL)
    y, zlo, core = r // 4, (r // 2) % 2, r % 2
    zhi, x = c // 4, c % 4
    hold = lax.optimization_barrier

    piece, pack, turned = prepare((r * 6).astype(jnp.int32).reshape(1), te, re, be, le, uc.T, rc.T, lc.T, tp.T, bp.T)
    swapped = swap_axes(turned)
    s2 = flat_form(hold((site_flat, turned))[0].reshape(13122, 128))
    swapped, s2 = hold((swapped, s2))
    piece, tpx, bpr = pieces(swapped, piece)

    piece = stacked(piece, [col_permute(piece, lambda z, i, s=s: ((z + s) % 4, i)) for s in (1, 2, 3)])
    piece = stacked(piece, [col_permute(piece, lambda z, i, s=s: (z, (i + s) % 4)) for s in (1, 2, 3)])
    at = jnp.arange(384)
    x_rel, z_rel, edge, j = at // 96, (at // 24) % 4, (at // 8) % 3, at % 8
    block = ((zhi - z_rel) % 4) * 4 + (x - x_rel) % 4
    target = jnp.where(j < 6, edge * 128 + block * 6 + j, -1)
    place = (target[:, None] == at[None, :]).astype(B)
    rows = lax.dot_general(piece, place, (((0,), (0,)), ((), ())), preferred_element_type=F).astype(B)
    ber = rows[:, 256:]

    own = jnp.concatenate([rows[:, :128], rows[:, 128:256], pack, tpx], axis=0)
    near = stacked(own, [other_z(own)])
    far = [along_y(near, s) for s in (1, 2, 3)]
    near_twin = other_core(near)
    wtop, wbot = left_forms(hold((s2, near))[0])
    *far, near_twin, wtop = hold((*far, near_twin, wtop))
    far_twin = [other_core(f) for f in far]
    bufs = [near, *far, near_twin, *far_twin]
    rel = jnp.arange(16)
    order = ((y - (rel // 2) % 4) % 4) * 4 + (zlo ^ (rel % 2)) * 2 + (core ^ (rel // 8))
    order = order.astype(jnp.int32)

    small = gather_small(order, bufs)

    lf, cb = left(order, bufs, small, ber, wtop, wbot, bpr)
    part = lambda v, n, size: lax.dynamic_slice_in_dim(v, n * size, size, 0)
    cb = part(cb, core, 64) + other_core(part(cb, 1 - core, 64))
    cb_z = other_z(part(cb, 1 - zlo, 32))
    wright = right_form(hold((s2, cb))[0])
    cb_z, wright = hold((cb_z, wright))
    cb = part(cb, zlo, 32) + cb_z
    cb_y = [along_y(part(cb, (y + s) % 4, 8), s) for s in (1, 2, 3)]
    order = hold((order, cb))[0]
    up, corner_top = upper(order, bufs, small, wtop, wright)
    *cb_y, up = hold((*cb_y, up))
    corner_bottom = finish(part(cb, y, 8), *cb_y)
    return up, lf, corner_top, corner_bottom


def solution(mesh):
    placed = (
        P(None, ROW),
        P(None, ROW),
        P(None, ROW),
        P(ROW, COL, None),
        P(ROW, COL, None),
        P(ROW, COL, None),
        P(ROW, COL, None),
        P(),
        P(COL, None),
        P(COL, None),
    )
    return jax.shard_map(
        shards,
        mesh=mesh,
        in_specs=placed,
        out_specs=(P(ROW, COL), P(COL, ROW), P(COL, ROW), P(COL, ROW)),
        check_vma=False,
    )
```

```python
import jax
import jax.numpy as jnp
from jax import lax
from jax.experimental import pallas as pl
from jax.experimental.pallas import tpu as pltpu
from jax.sharding import PartitionSpec as P

F = jnp.float32
B = jnp.bfloat16
NN = (((1,), (0,)), ((), ()))
NT = (((1,), (1,)), ((), ()))
VM = pl.BlockSpec(memory_space=pltpu.VMEM)
SM = pl.BlockSpec(memory_space=pltpu.SMEM)
HB = pl.BlockSpec(memory_space=pltpu.HBM)
BLOCK = 496
WIDE = 3456


def dot(x, y, dims=NN):
    return lax.dot_general(x, y, dims, preferred_element_type=F)


def shape_of(*dims, kind=B):
    return jax.ShapeDtypeStruct(dims, kind)


def params(mib):
    return pltpu.CompilerParams(vmem_limit_bytes=mib << 20)


def work(flops):
    return pl.CostEstimate(flops=flops, transcendentals=0, bytes_accessed=1 << 22)


def load(pairs, sems):
    copies = [pltpu.make_async_copy(src, dst, sems.at[n]) for n, (src, dst) in enumerate(pairs)]
    for cp in copies:
        cp.start()
    return copies


def prepare_kernel(at_ref, *refs):
    hbm, (piece, pack, turned), local, sems = refs[:9], refs[9:12], refs[12:21], refs[21]
    for cp in load(list(zip(hbm, local)), sems):
        cp.wait()
    te, re, be, le, uct, rct, lct, tpt, bpt = local
    zero = jnp.zeros((2, 216), B)
    for n, e in ((0, te), (1, le)):
        v = e[...].astype(F)
        piece[8 * n:8 * n + 8, :] = jnp.concatenate(
            [jnp.concatenate([v[i] for i in range(6)], axis=1).astype(B), zero], axis=0)
    parts = []
    for e in (te, re, be):
        v = e[...].astype(F)
        parts.append(jnp.concatenate([v[:, j, :] for j in range(6)], axis=1))
    bottom = parts.pop()
    row = lax.broadcasted_iota(jnp.int32, (8, 96), 0)
    lane = lax.broadcasted_iota(jnp.int32, (8, 96), 1)
    pick = ((lane == at_ref[0] + row) & (row < 6)).astype(B)
    turned[0:8, :] = dot(pick, tpt[...]).astype(B)
    turned[8:16, :] = dot(pick, bpt[...]).astype(B)
    turned[16:24, :] = jnp.concatenate([bottom.astype(B), zero], axis=0)
    for c in (uct, rct, lct):
        parts.append(c[...].astype(F))
    flat = jnp.concatenate(parts + [jnp.zeros((6, 48), F)], axis=1)
    flat = jnp.concatenate([flat, jnp.zeros((2, 768), F)], axis=0).astype(B)
    for k in range(6):
        pack[8 * k:8 * k + 8, :] = flat[:, 128 * k:128 * k + 128]


def pieces_kernel(turned, piece, out, tpx, bpr):
    out[0:16, :] = piece[...]
    out[16:24, :] = turned[16:24, :]
    top = turned[0:8, :].astype(F)
    flat = jnp.concatenate(
        [jnp.concatenate([top[x:x + 1, b * 36:(b + 1) * 36] for x in range(6)], axis=1) for b in range(6)], axis=0)
    flat = jnp.concatenate([flat, jnp.zeros((6, 40), F)], axis=1)
    flat = jnp.concatenate([flat, jnp.zeros((2, 256), F)], axis=0).astype(B)
    tpx[0:8, :] = flat[:, :128]
    tpx[8:16, :] = flat[:, 128:]
    bottom = turned[8:16, :].astype(F)
    gap = jnp.zeros((8, 4), F)
    bpr[...] = jnp.concatenate([y for b in range(6) for y in (bottom[:, b * 36:(b + 1) * 36], gap)], axis=1).astype(B)


def expand(order_ref, bufs, off, dst):
    for rel in range(16):
        at = pl.multiple_of(order_ref[rel] * 216, 8)
        start = (rel % 2) * BLOCK + off
        dst[pl.ds(at, 216), :] = bufs[rel // 2][start:start + 216, :].astype(F)


def gather_small_kernel(order_ref, *refs):
    bufs = refs[:8]
    out_ref, packs = refs[8:]
    for rel in range(16):
        at = pl.multiple_of(order_ref[rel] * 8, 8)
        start = (rel % 2) * BLOCK + 432
        for k in range(8):
            packs[k, pl.ds(at, 8), :] = bufs[rel // 2][start + 8 * k:start + 8 * k + 8, :].astype(F)
    row = lax.broadcasted_iota(jnp.int32, (128, 128), 0)
    lane = lax.broadcasted_iota(jnp.int32, (128, 128), 1)
    place = ((row % 8 < 6) & (lane == (row // 8) * 6 + row % 8)).astype(B)
    for k in range(8):
        out_ref[k * 128:(k + 1) * 128, :] = dot(jnp.transpose(packs[k]).astype(B), place).astype(B)


def gather_small(order, bufs):
    return pl.pallas_call(gather_small_kernel, out_shape=shape_of(1024, 128), in_specs=[SM] + [VM] * 8, out_specs=VM,
                          scratch_shapes=[pltpu.VMEM((8, 128, 128), F)], name="gather_small",
                          compiler_params=params(6))(order, *bufs)


def to_bf16(src, dst, rows):
    def f(i, _):
        at = pl.multiple_of(i * 48, 16)
        for a in range(6):
            dst[pl.ds(at, 48), a * 128:(a + 1) * 128] = src[a, pl.ds(at, 48), :].astype(B)
        return 0
    lax.fori_loop(0, rows // 48, f, 0)


def big(w_ref, p_ref, k, o_ref):
    def f(i, _):
        at = pl.multiple_of(i * 432, 16)
        res = dot(w_ref[pl.ds(at, 432), :k], p_ref[:k, :])
        for a in range(6):
            o_ref[a, pl.ds(at, 432), :] = res[:, a * 128:(a + 1) * 128]
        return 0
    lax.fori_loop(0, 3, f, 0)
    o_ref[:, 1296:1440, :] = jnp.zeros((6, 144, 128), F)


def padded(x):
    return jnp.concatenate([x, jnp.zeros((x.shape[0], 32), F)], axis=1)


def clear_gaps(pf):
    for q in range(12):
        pf[:, q * 128 + 108:(q + 1) * 128, :] = jnp.zeros((6, 20, 128), F)


def compressed(x):
    return jnp.concatenate([x[:, g * 40:g * 40 + 36] for g in range(6)], axis=1)


def upper_kernel(order_ref, *refs):
    bufs = refs[:8]
    small_ref, wtop_hbm, wright_hbm, out_ref, ct_ref, tef, pf, p1, p3, o1, o3, tps, wtop_ref, wright_ref, sems = refs[8:]
    copies = load([(wtop_hbm, wtop_ref), (wright_hbm, wright_ref)], sems)
    expand(order_ref, bufs, 0, tef)
    uc = small_ref[432:528, :]
    rc = small_ref[528:624, :]
    tps[0:216, :] = small_ref[768:984, :].astype(F)
    tps[216:320, :] = jnp.zeros((104, 128), F)
    lu = dot(bufs[0][216:432, :][:, :96], uc).astype(B)[:, :96]
    ar = dot(small_ref[216:432, :], rc, NT).astype(B)
    for v in range(36):
        te = tef[pl.ds(v, 96, stride=36), :].astype(B)
        d1 = dot(lu, te)
        for a in range(6):
            pf[a, v * 36:(v + 1) * 36, :] = d1[a * 36:(a + 1) * 36, :]
    to_bf16(pf, p1, 1296)
    clear_gaps(pf)
    for v in range(36):
        te = tef[pl.ds(v, 96, stride=36), :].astype(B)
        d3 = padded(dot(ar, te[:, :96], NT))
        at = (v // 3) * 128 + (v % 3) * 36
        for a in range(6):
            pf[a, at:at + 36, :] = d3[a * 36:(a + 1) * 36, :]
    to_bf16(pf, p3, 1536)
    copies[0].wait()
    big(wtop_ref, p1, 1296, o1)
    copies[1].wait()
    big(wright_ref, p3, 1536, o3)
    acc = jnp.zeros((240, 256), F)
    for tp in range(18):
        xs = []
        ys = []
        for t in (2 * tp, 2 * tp + 1):
            xs.append(jnp.concatenate([o1[a, pl.ds(t, 40, stride=36), :] for a in range(6)], axis=0).astype(B))
            ys.append(jnp.concatenate([o3[g, pl.ds(t, 40, stride=36), :] for g in range(6)]
                                      + [tps[pl.ds(t, 8, stride=36), :], jnp.zeros((8, 128), F)], axis=0).astype(B))
        acc = acc + dot(jnp.concatenate(xs, axis=1), jnp.concatenate(ys, axis=1), NT)
    up = compressed(acc[:, :240] * jnp.float32(WIDE ** -0.5))
    for a in range(6):
        out_ref[a * 36:(a + 1) * 36, :] = up[a * 40:a * 40 + 36, :].astype(B)
    ct = jnp.transpose(acc[:, 128:256])[112:120, :]
    ct_ref[...] = compressed(ct)[0:6, :].astype(B)


def left_kernel(order_ref, *refs):
    bufs = refs[:8]
    small_ref, ber_ref, wtop_hbm, wbot_hbm, bpr_ref, out_ref, cb_ref, lef, pf, p2, p4, o2, o4, cbs, wtop_ref, wbot_ref, sems = refs[8:]
    copies = load([(wtop_hbm, wtop_ref), (wbot_hbm, wbot_ref)], sems)
    expand(order_ref, bufs, 216, lef)
    uc = small_ref[432:528, :]
    lc = small_ref[624:720, :]
    at = dot(small_ref[0:216, :], uc, NT).astype(B)
    ab = dot(ber_ref[...], lc, NT).astype(B)[:, :96]
    for u in range(36):
        le = lef[pl.ds(u, 96, stride=36), :].astype(B)
        d2 = padded(dot(at, le[:, :96], NT))
        for b in range(6):
            pf[b, u * 36:(u + 1) * 36, :] = d2[b * 36:(b + 1) * 36, :]
    for g in range(9):
        for b in range(6):
            p2[g * 144:(g + 1) * 144, b * 128:(b + 1) * 128] = jnp.concatenate(
                [pf[b, pl.ds(4 * g + e, 36, stride=36), :] for e in range(4)], axis=0).astype(B)
    for u in range(36):
        le = lef[pl.ds(u, 96, stride=36), :].astype(B)
        d4 = dot(ab, le)
        for b in range(6):
            pf[b, u * 36:(u + 1) * 36, :] = d4[b * 36:(b + 1) * 36, :]
    gap = jnp.zeros((20, 128), F)
    for q in range(12):
        for b in range(6):
            p4[q * 128:(q + 1) * 128, b * 128:(b + 1) * 128] = jnp.concatenate(
                [pf[b, pl.ds(3 * q + e, 36, stride=36), :] for e in range(3)] + [gap], axis=0).astype(B)
    copies[0].wait()
    big(wtop_ref, p2, 1296, o2)
    copies[1].wait()
    big(wbot_ref, p4, 1536, o4)
    acc = jnp.zeros((240, 240), F)
    for sp in range(18):
        xs = []
        ys = []
        for s in (2 * sp, 2 * sp + 1):
            x = jnp.concatenate([o2[b, s * 36:s * 36 + 40, :] for b in range(6)], axis=0).astype(B)
            y = jnp.concatenate([o4[b, s * 36:s * 36 + 40, :] for b in range(6)], axis=0).astype(B)
            xs.append(x)
            ys.append(y)
            cbs[pl.ds(s, 8, stride=36), :] = dot(bpr_ref[...], y)
        acc = acc + dot(jnp.concatenate(xs, axis=1), jnp.concatenate(ys, axis=1), NT)
    lh = compressed(acc * jnp.float32(WIDE ** -0.5))
    for a in range(6):
        out_ref[a * 36:(a + 1) * 36, :] = lh[a * 40:a * 40 + 36, :].astype(B)
    sums = jnp.transpose(cbs[0:256, :])
    cb_ref[...] = jnp.zeros((128, 256), F)
    for m in range(16):
        at = ((m % 4) * 4 + ((m // 4) % 2) * 2 + m // 8) * 6
        cb_ref[8 * m:8 * m + 6, :] = sums[at:at + 6, :]


def scratch():
    return [pltpu.VMEM((WIDE, 128), F), pltpu.VMEM((6, 2048, 128), F), pltpu.VMEM((1536, 768), B),
            pltpu.VMEM((1536, 768), B), pltpu.VMEM((6, 1440, 128), F), pltpu.VMEM((6, 1440, 128), F)]


def prepare(at, *args):
    return pl.pallas_call(
        prepare_kernel, out_shape=(shape_of(16, 216), shape_of(48, 128), shape_of(24, 216)),
        in_specs=[SM] + [HB] * 9, out_specs=(VM,) * 3,
        scratch_shapes=[pltpu.VMEM(x.shape, B) for x in args] + [pltpu.SemaphoreType.DMA((9,))],
        name="prepare")(at, *args)


def pieces(turned, piece):
    return pl.pallas_call(pieces_kernel, out_shape=(shape_of(24, 216), shape_of(16, 128), shape_of(8, 240)),
                          in_specs=[VM, VM], out_specs=(VM,) * 3, name="pieces",
                          compiler_params=params(4))(turned, piece)


def form_copies():
    return [pltpu.VMEM((1296, 1408), B), pltpu.VMEM((1296, 1536), B), pltpu.SemaphoreType.DMA((2,))]


def upper(order, bufs, small, wtop, wright):
    return pl.pallas_call(
        upper_kernel, out_shape=(shape_of(216, 216), shape_of(6, 216)), in_specs=[SM] + [VM] * 9 + [HB] * 2,
        out_specs=(VM, VM), scratch_shapes=scratch() + [pltpu.VMEM((320, 128), F)] + form_copies(), name="upper",
        compiler_params=params(50), cost_estimate=work(8 << 30))(order, *bufs, small, wtop, wright)


def left(order, bufs, small, ber, wtop, wbot, bpr):
    return pl.pallas_call(
        left_kernel, out_shape=(shape_of(216, 216), shape_of(128, 256, kind=F)),
        in_specs=[SM] + [VM] * 10 + [HB] * 2 + [VM], out_specs=(VM, VM),
        scratch_shapes=scratch() + [pltpu.VMEM((288, 128), F)] + form_copies(), name="left",
        compiler_params=params(50), cost_estimate=work(8 << 30))(order, *bufs, small, ber, wtop, wbot, bpr)


def finish_kernel(own, one, two, three, out_ref):
    res = own[...] + one[...] + two[...] + three[...]
    rows = [jnp.concatenate([res[a:a + 1, x * 36:(x + 1) * 36] for a in range(6)], axis=1) for x in range(6)]
    out_ref[...] = jnp.concatenate(rows, axis=0).astype(B)


def finish(*parts):
    return pl.pallas_call(finish_kernel, out_shape=shape_of(6, 216), in_specs=[VM] * 4, out_specs=VM,
                          name="finish", compiler_params=params(4))(*parts)


def lane_pattern(ref):
    k = lax.broadcasted_iota(jnp.int32, (256, 256), 0)
    n = lax.broadcasted_iota(jnp.int32, (256, 256), 1)
    w = n % 128
    ref[...] = jnp.where(w < 108, k - (n // 128) * 36 - w % 36, -1)


def lanes_shifted(a_ref, z_ref, pattern, pair):
    tile = (pair * 72) // 128
    base = pl.multiple_of(tile * 128, 128)
    off = pair * 72 - tile * 128
    sel = (pattern[...] == off).astype(B)
    z_ref[...] = dot(a_ref[:, pl.ds(base, 256)], sel)


def column_chunks(src, dst, sems):
    ends = (0, 384, 768, 1152, 1408)
    return load([(src.at[:, p:q], dst.at[:, p:q]) for p, q in zip(ends, ends[1:])], sems)


def realign(a_ref, z_ref, o_ref, pattern, out_hbm, sem, chunks=()):
    lane = lax.broadcasted_iota(jnp.int32, (36, 128), 1)

    def f(g, _):
        for n, cp in zip((0, 2, 4, 7), chunks):
            @pl.when(g == n)
            def _(cp=cp):
                cp.wait()
        strips = []
        for h in range(2):
            lanes_shifted(a_ref, z_ref.at[h], pattern, 2 * g + h)
        for h in range(2):
            for q in range(2):
                tiles = []
                for m in range(12):
                    z = [z_ref[h, (3 * m + e) * 36:(3 * m + e + 1) * 36, q * 128:(q + 1) * 128] for e in range(3)]
                    tiles.append(jnp.where(lane < 36, z[0], jnp.where(lane < 72, z[1], z[2])))
                strips.append(jnp.concatenate(tiles, axis=1))
        at = pl.multiple_of(g * 144, 16)
        o_ref[pl.ds(at, 144), :] = jnp.concatenate(strips, axis=0).astype(B)
        pltpu.make_async_copy(o_ref.at[pl.ds(at, 144), :], out_hbm.at[pl.ds(at, 144), :], sem.at[g]).start()
        return 0
    lax.fori_loop(0, 9, f, 0)

    def w(g, _):
        at = pl.multiple_of(g * 144, 16)
        pltpu.make_async_copy(o_ref.at[pl.ds(at, 144), :], out_hbm.at[pl.ds(at, 144), :], sem.at[g]).wait()
        return 0
    lax.fori_loop(0, 9, w, 0)


def right_form_kernel(s_hbm, wright_hbm, apad, z, o, pattern, sems, done):
    chunks = column_chunks(s_hbm, apad, sems)
    lane_pattern(pattern)
    realign(apad, z, o, pattern, wright_hbm, done, chunks)


def left_forms_kernel(s_hbm, wtop_hbm, wbot_hbm, apad, z, o, pattern, sems, done, s_ref):
    chunks = column_chunks(s_hbm, s_ref, sems)
    lane_pattern(pattern)
    eye = (lax.broadcasted_iota(jnp.int32, (128, 128), 0) == lax.broadcasted_iota(jnp.int32, (128, 128), 1)).astype(B)
    for b in range(11):
        n = min(128, 1296 - b * 128)
        if b % 3 == 0:
            chunks[b // 3].wait()
        apad[b * 128:b * 128 + n, :1296] = dot(eye[:n, :n], s_ref[:, b * 128:b * 128 + n], NT).astype(B)
    apad[:, 1296:1408] = jnp.zeros((1296, 112), B)
    out = pltpu.make_async_copy(apad, wtop_hbm, sems.at[0])
    out.start()
    realign(apad, z, o, pattern, wbot_hbm, done)
    out.wait()


def flat_form_kernel(x_ref, s_hbm, wide, tiles, s_ref, sems):
    def widen(i, _):
        at = pl.multiple_of(i * 256, 16)
        wide[pl.ds(at, 256), :] = x_ref[pl.ds(at, 256), :].astype(F)
        return 0
    lax.fori_loop(0, 51, widen, 0)
    wide[13056:13122, :] = x_ref[13056:13122, :].astype(F)
    lane = lax.broadcasted_iota(jnp.int32, (162, 128), 1)
    for i in range(8):
        def turn(j):
            v = wide[pl.ds(10 * i + j, 162, stride=81), :]
            return pltpu.roll(v, 128 - 16 * i, 1) if i else v
        here = turn(0)
        for j in range(11):
            if j == 10:
                tile = jnp.where(lane < 16, here, 0.0)
            else:
                after = turn(j + 1)
                tile = jnp.where(lane < 128 - 16 * i, here, after) if i else here
                here = after
            tiles[j, pl.ds(i, 162, stride=8), :] = tile

    def narrow(g, _):
        at = pl.multiple_of(g * 144, 16)
        for j in range(11):
            s_ref[pl.ds(at, 144), 128 * j:128 * j + 128] = tiles[j, pl.ds(at, 144), :].astype(B)
        pltpu.make_async_copy(s_ref.at[pl.ds(at, 144), :], s_hbm.at[pl.ds(at, 144), :], sems.at[g]).start()
        return 0
    lax.fori_loop(0, 9, narrow, 0)

    def w(g, _):
        at = pl.multiple_of(g * 144, 16)
        pltpu.make_async_copy(s_ref.at[pl.ds(at, 144), :], s_hbm.at[pl.ds(at, 144), :], sems.at[g]).wait()
        return 0
    lax.fori_loop(0, 9, w, 0)


def form_scratch():
    return [pltpu.VMEM((1296, 1408), B), pltpu.VMEM((2, 1296, 256), F), pltpu.VMEM((1296, 1536), B),
            pltpu.VMEM((256, 256), jnp.int32),
            pltpu.SemaphoreType.DMA((4,)), pltpu.SemaphoreType.DMA((9,))]


def flat_form(flat):
    return pl.pallas_call(flat_form_kernel, out_shape=shape_of(1296, 1408), in_specs=[VM], out_specs=HB,
                          scratch_shapes=[pltpu.VMEM((13616, 128), F), pltpu.VMEM((11, 1344, 128), F),
                                          pltpu.VMEM((1296, 1408), B), pltpu.SemaphoreType.DMA((9,))],
                          name="flat_form", compiler_params=params(60), cost_estimate=work(3 << 30))(flat)


def right_form(s2):
    return pl.pallas_call(right_form_kernel, out_shape=shape_of(1296, 1536), in_specs=[HB], out_specs=HB,
                          scratch_shapes=form_scratch(), name="right_form", compiler_params=params(60),
                          cost_estimate=work(3 << 30))(s2)


def left_forms(s2):
    return pl.pallas_call(left_forms_kernel, out_shape=(shape_of(1296, 1408), shape_of(1296, 1536)), in_specs=[HB],
                          out_specs=(HB, HB), scratch_shapes=form_scratch() + [pltpu.VMEM((1296, 1408), B)],
                          name="left_forms", compiler_params=params(60), cost_estimate=work(4 << 30))(s2)


ROW, COL = "row", "col"


def row_permute(x, move):
    pairs = []
    for y in range(4):
        for z in range(2):
            for k in range(2):
                a, b, c = move(y, z, k)
                pairs.append((y * 4 + z * 2 + k, a * 4 + b * 2 + c))
    return lax.ppermute(x, ROW, pairs)


def col_permute(x, move):
    pairs = []
    for z in range(4):
        for i in range(4):
            a, b = move(z, i)
            pairs.append((z * 4 + i, a * 4 + b))
    return lax.ppermute(x, COL, pairs)


def swap_axes(x):
    pairs = [(r * 16 + c, c * 16 + r) for r in range(16) for c in range(16)]
    return lax.ppermute(x, (ROW, COL), pairs)


def stacked(own, received):
    return jnp.concatenate([own, *received], axis=0)


def other_core(x):
    return row_permute(x, lambda a, b, k: (a, b, 1 - k))


def other_z(x):
    return row_permute(x, lambda a, b, k: (a, 1 - b, k))


def along_y(x, s):
    return row_permute(x, lambda a, b, k: ((a + s) % 4, b, k))


def shards(uc, rc, lc, te, re, be, le, site_flat, tp, bp):
    r = lax.axis_index(ROW)
    c = lax.axis_index(COL)
    y, zlo, core = r // 4, (r // 2) % 2, r % 2
    zhi, x = c // 4, c % 4
    hold = lax.optimization_barrier

    piece, pack, turned = prepare((r * 6).astype(jnp.int32).reshape(1), te, re, be, le, uc.T, rc.T, lc.T, tp.T, bp.T)
    swapped = swap_axes(turned)
    s2 = flat_form(hold((site_flat, turned))[0].reshape(13122, 128))
    swapped, s2 = hold((swapped, s2))
    piece, tpx, bpr = pieces(swapped, piece)

    piece = stacked(piece, [col_permute(piece, lambda z, i, s=s: ((z + s) % 4, i)) for s in (1, 2, 3)])
    piece = stacked(piece, [col_permute(piece, lambda z, i, s=s: (z, (i + s) % 4)) for s in (1, 2, 3)])
    at = jnp.arange(384)
    x_rel, z_rel, edge, j = at // 96, (at // 24) % 4, (at // 8) % 3, at % 8
    block = ((zhi - z_rel) % 4) * 4 + (x - x_rel) % 4
    target = jnp.where(j < 6, edge * 128 + block * 6 + j, -1)
    place = (target[:, None] == at[None, :]).astype(B)
    rows = lax.dot_general(piece, place, (((0,), (0,)), ((), ())), preferred_element_type=F).astype(B)
    ber = rows[:, 256:]

    own = jnp.concatenate([rows[:, :128], rows[:, 128:256], pack, tpx], axis=0)
    near = stacked(own, [other_z(own)])
    far = [along_y(near, s) for s in (1, 2, 3)]
    near_twin = other_core(near)
    wtop, wbot = left_forms(hold((s2, near))[0])
    *far, near_twin, wtop = hold((*far, near_twin, wtop))
    far_twin = [other_core(f) for f in far]
    bufs = [near, *far, near_twin, *far_twin]
    rel = jnp.arange(16)
    order = ((y - (rel // 2) % 4) % 4) * 4 + (zlo ^ (rel % 2)) * 2 + (core ^ (rel // 8))
    order = order.astype(jnp.int32)

    small = gather_small(order, bufs)

    lf, cb = left(order, bufs, small, ber, wtop, wbot, bpr)
    part = lambda v, n, size: lax.dynamic_slice_in_dim(v, n * size, size, 0)
    cb = part(cb, core, 64) + other_core(part(cb, 1 - core, 64))
    cb_z = other_z(part(cb, 1 - zlo, 32))
    wright = right_form(hold((s2, cb))[0])
    cb_z, wright = hold((cb_z, wright))
    cb = part(cb, zlo, 32) + cb_z
    cb_y = [along_y(part(cb, (y + s) % 4, 8), s) for s in (1, 2, 3)]
    order = hold((order, cb))[0]
    up, corner_top = upper(order, bufs, small, wtop, wright)
    *cb_y, up = hold((*cb_y, up))
    corner_bottom = finish(part(cb, y, 8), *cb_y)
    return up, lf, corner_top, corner_bottom


def solution(mesh):
    placed = (
        P(None, ROW),
        P(None, ROW),
        P(None, ROW),
        P(ROW, COL, None),
        P(ROW, COL, None),
        P(ROW, COL, None),
        P(ROW, COL, None),
        P(),
        P(COL, None),
        P(COL, None),
    )
    return jax.shard_map(
        shards,
        mesh=mesh,
        in_specs=placed,
        out_specs=(P(ROW, COL), P(COL, ROW), P(COL, ROW), P(COL, ROW)),
        check_vma=False,
    )
```

```python
import jax
import jax.numpy as jnp
from jax import lax
from jax.experimental import pallas as pl
from jax.experimental.pallas import tpu as pltpu
from jax.sharding import PartitionSpec as P

F = jnp.float32
B = jnp.bfloat16
NN = (((1,), (0,)), ((), ()))
NT = (((1,), (1,)), ((), ()))
VM = pl.BlockSpec(memory_space=pltpu.VMEM)
SM = pl.BlockSpec(memory_space=pltpu.SMEM)
HB = pl.BlockSpec(memory_space=pltpu.HBM)
BLOCK = 496
WIDE = 3456


def dot(x, y, dims=NN):
    return lax.dot_general(x, y, dims, preferred_element_type=F)


def shape_of(*dims, kind=B):
    return jax.ShapeDtypeStruct(dims, kind)


def params(mib):
    return pltpu.CompilerParams(vmem_limit_bytes=mib << 20)


def work(flops):
    return pl.CostEstimate(flops=flops, transcendentals=0, bytes_accessed=1 << 22)


def load(pairs, sems):
    copies = [pltpu.make_async_copy(src, dst, sems.at[n]) for n, (src, dst) in enumerate(pairs)]
    for cp in copies:
        cp.start()
    return copies


def prepare_kernel(at_ref, *refs):
    hbm, (piece, pack, turned), local, sems = refs[:9], refs[9:12], refs[12:21], refs[21]
    for cp in load(list(zip(hbm, local)), sems):
        cp.wait()
    te, re, be, le, uct, rct, lct, tpt, bpt = local
    zero = jnp.zeros((2, 216), B)
    for n, e in ((0, te), (1, le)):
        v = e[...].astype(F)
        piece[8 * n:8 * n + 8, :] = jnp.concatenate(
            [jnp.concatenate([v[i] for i in range(6)], axis=1).astype(B), zero], axis=0)
    parts = []
    for e in (te, re, be):
        v = e[...].astype(F)
        parts.append(jnp.concatenate([v[:, j, :] for j in range(6)], axis=1))
    bottom = parts.pop()
    row = lax.broadcasted_iota(jnp.int32, (8, 96), 0)
    lane = lax.broadcasted_iota(jnp.int32, (8, 96), 1)
    pick = ((lane == at_ref[0] + row) & (row < 6)).astype(B)
    turned[0:8, :] = dot(pick, tpt[...]).astype(B)
    turned[8:16, :] = dot(pick, bpt[...]).astype(B)
    turned[16:24, :] = jnp.concatenate([bottom.astype(B), zero], axis=0)
    for c in (uct, rct, lct):
        parts.append(c[...].astype(F))
    flat = jnp.concatenate(parts + [jnp.zeros((6, 48), F)], axis=1)
    flat = jnp.concatenate([flat, jnp.zeros((2, 768), F)], axis=0).astype(B)
    for k in range(6):
        pack[8 * k:8 * k + 8, :] = flat[:, 128 * k:128 * k + 128]


def pieces_kernel(turned, piece, out, tpx, bpr):
    out[0:16, :] = piece[...]
    out[16:24, :] = turned[16:24, :]
    top = turned[0:8, :].astype(F)
    flat = jnp.concatenate(
        [jnp.concatenate([top[x:x + 1, b * 36:(b + 1) * 36] for x in range(6)], axis=1) for b in range(6)], axis=0)
    flat = jnp.concatenate([flat, jnp.zeros((6, 40), F)], axis=1)
    flat = jnp.concatenate([flat, jnp.zeros((2, 256), F)], axis=0).astype(B)
    tpx[0:8, :] = flat[:, :128]
    tpx[8:16, :] = flat[:, 128:]
    bottom = turned[8:16, :].astype(F)
    gap = jnp.zeros((8, 4), F)
    bpr[...] = jnp.concatenate([y for b in range(6) for y in (bottom[:, b * 36:(b + 1) * 36], gap)], axis=1).astype(B)


def expand(order_ref, bufs, off, dst):
    for rel in range(16):
        at = pl.multiple_of(order_ref[rel] * 216, 8)
        start = (rel % 2) * BLOCK + off
        dst[pl.ds(at, 216), :] = bufs[rel // 2][start:start + 216, :].astype(F)


def gather_small_kernel(order_ref, *refs):
    bufs = refs[:8]
    out_ref, packs = refs[8:]
    for rel in range(16):
        at = pl.multiple_of(order_ref[rel] * 8, 8)
        start = (rel % 2) * BLOCK + 432
        for k in range(8):
            packs[k, pl.ds(at, 8), :] = bufs[rel // 2][start + 8 * k:start + 8 * k + 8, :].astype(F)
    row = lax.broadcasted_iota(jnp.int32, (128, 128), 0)
    lane = lax.broadcasted_iota(jnp.int32, (128, 128), 1)
    place = ((row % 8 < 6) & (lane == (row // 8) * 6 + row % 8)).astype(B)
    for k in range(8):
        out_ref[k * 128:(k + 1) * 128, :] = dot(jnp.transpose(packs[k]).astype(B), place).astype(B)


def gather_small(order, bufs):
    return pl.pallas_call(gather_small_kernel, out_shape=shape_of(1024, 128), in_specs=[SM] + [VM] * 8, out_specs=VM,
                          scratch_shapes=[pltpu.VMEM((8, 128, 128), F)], name="gather_small",
                          compiler_params=params(6))(order, *bufs)


def to_bf16(src, dst, rows):
    def f(i, _):
        at = pl.multiple_of(i * 48, 16)
        for a in range(6):
            dst[pl.ds(at, 48), a * 128:(a + 1) * 128] = src[a, pl.ds(at, 48), :].astype(B)
        return 0
    lax.fori_loop(0, rows // 48, f, 0)


def big(w_ref, p_ref, k, o_ref):
    def f(i, _):
        at = pl.multiple_of(i * 432, 16)
        res = dot(w_ref[pl.ds(at, 432), :k], p_ref[:k, :])
        for a in range(6):
            o_ref[a, pl.ds(at, 432), :] = res[:, a * 128:(a + 1) * 128]
        return 0
    lax.fori_loop(0, 3, f, 0)
    o_ref[:, 1296:1440, :] = jnp.zeros((6, 144, 128), F)


def padded(x):
    return jnp.concatenate([x, jnp.zeros((x.shape[0], 32), F)], axis=1)


def clear_gaps(pf):
    for q in range(12):
        pf[:, q * 128 + 108:(q + 1) * 128, :] = jnp.zeros((6, 20, 128), F)


def compressed(x):
    return jnp.concatenate([x[:, g * 40:g * 40 + 36] for g in range(6)], axis=1)


def upper_kernel(order_ref, *refs):
    bufs = refs[:8]
    small_ref, wtop_hbm, wright_hbm, out_ref, ct_ref, tef, pf, p1, p3, o1, o3, tps, wtop_ref, wright_ref, sems = refs[8:]
    copies = load([(wtop_hbm, wtop_ref), (wright_hbm, wright_ref)], sems)
    expand(order_ref, bufs, 0, tef)
    uc = small_ref[432:528, :]
    rc = small_ref[528:624, :]
    tps[0:216, :] = small_ref[768:984, :].astype(F)
    tps[216:320, :] = jnp.zeros((104, 128), F)
    lu = dot(bufs[0][216:432, :][:, :96], uc).astype(B)[:, :96]
    ar = dot(small_ref[216:432, :], rc, NT).astype(B)
    for v in range(36):
        te = tef[pl.ds(v, 96, stride=36), :].astype(B)
        d1 = dot(lu, te)
        for a in range(6):
            pf[a, v * 36:(v + 1) * 36, :] = d1[a * 36:(a + 1) * 36, :]
    to_bf16(pf, p1, 1296)
    clear_gaps(pf)
    for v in range(36):
        te = tef[pl.ds(v, 96, stride=36), :].astype(B)
        d3 = padded(dot(ar, te[:, :96], NT))
        at = (v // 3) * 128 + (v % 3) * 36
        for a in range(6):
            pf[a, at:at + 36, :] = d3[a * 36:(a + 1) * 36, :]
    to_bf16(pf, p3, 1536)
    copies[0].wait()
    big(wtop_ref, p1, 1296, o1)
    copies[1].wait()
    big(wright_ref, p3, 1536, o3)
    acc = jnp.zeros((240, 256), F)
    for tp in range(18):
        xs = []
        ys = []
        for t in (2 * tp, 2 * tp + 1):
            xs.append(jnp.concatenate([o1[a, pl.ds(t, 40, stride=36), :] for a in range(6)], axis=0).astype(B))
            ys.append(jnp.concatenate([o3[g, pl.ds(t, 40, stride=36), :] for g in range(6)]
                                      + [tps[pl.ds(t, 8, stride=36), :], jnp.zeros((8, 128), F)], axis=0).astype(B))
        acc = acc + dot(jnp.concatenate(xs, axis=1), jnp.concatenate(ys, axis=1), NT)
    up = compressed(acc[:, :240] * jnp.float32(WIDE ** -0.5))
    for a in range(6):
        out_ref[a * 36:(a + 1) * 36, :] = up[a * 40:a * 40 + 36, :].astype(B)
    ct = jnp.transpose(acc[:, 128:256])[112:120, :]
    ct_ref[...] = compressed(ct)[0:6, :].astype(B)


def left_kernel(order_ref, *refs):
    bufs = refs[:8]
    small_ref, ber_ref, wtop_hbm, wbot_hbm, bpr_ref, out_ref, cb_ref, lef, pf, p2, p4, o2, o4, cbs, wtop_ref, wbot_ref, sems = refs[8:]
    copies = load([(wtop_hbm, wtop_ref), (wbot_hbm, wbot_ref)], sems)
    expand(order_ref, bufs, 216, lef)
    uc = small_ref[432:528, :]
    lc = small_ref[624:720, :]
    at = dot(small_ref[0:216, :], uc, NT).astype(B)
    ab = dot(ber_ref[...], lc, NT).astype(B)[:, :96]
    for u in range(36):
        le = lef[pl.ds(u, 96, stride=36), :].astype(B)
        d2 = padded(dot(at, le[:, :96], NT))
        for b in range(6):
            pf[b, u * 36:(u + 1) * 36, :] = d2[b * 36:(b + 1) * 36, :]
    for g in range(9):
        for b in range(6):
            p2[g * 144:(g + 1) * 144, b * 128:(b + 1) * 128] = jnp.concatenate(
                [pf[b, pl.ds(4 * g + e, 36, stride=36), :] for e in range(4)], axis=0).astype(B)
    for u in range(36):
        le = lef[pl.ds(u, 96, stride=36), :].astype(B)
        d4 = dot(ab, le)
        for b in range(6):
            pf[b, u * 36:(u + 1) * 36, :] = d4[b * 36:(b + 1) * 36, :]
    gap = jnp.zeros((20, 128), F)
    for q in range(12):
        for b in range(6):
            p4[q * 128:(q + 1) * 128, b * 128:(b + 1) * 128] = jnp.concatenate(
                [pf[b, pl.ds(3 * q + e, 36, stride=36), :] for e in range(3)] + [gap], axis=0).astype(B)
    copies[0].wait()
    big(wtop_ref, p2, 1296, o2)
    copies[1].wait()
    big(wbot_ref, p4, 1536, o4)
    acc = jnp.zeros((240, 240), F)
    for sp in range(18):
        xs = []
        ys = []
        for s in (2 * sp, 2 * sp + 1):
            x = jnp.concatenate([o2[b, s * 36:s * 36 + 40, :] for b in range(6)], axis=0).astype(B)
            y = jnp.concatenate([o4[b, s * 36:s * 36 + 40, :] for b in range(6)], axis=0).astype(B)
            xs.append(x)
            ys.append(y)
            cbs[pl.ds(s, 8, stride=36), :] = dot(bpr_ref[...], y)
        acc = acc + dot(jnp.concatenate(xs, axis=1), jnp.concatenate(ys, axis=1), NT)
    lh = compressed(acc * jnp.float32(WIDE ** -0.5))
    for a in range(6):
        out_ref[a * 36:(a + 1) * 36, :] = lh[a * 40:a * 40 + 36, :].astype(B)
    sums = jnp.transpose(cbs[0:256, :])
    cb_ref[...] = jnp.zeros((128, 256), F)
    for m in range(16):
        at = ((m % 4) * 4 + ((m // 4) % 2) * 2 + m // 8) * 6
        cb_ref[8 * m:8 * m + 6, :] = sums[at:at + 6, :]


def scratch():
    return [pltpu.VMEM((WIDE, 128), F), pltpu.VMEM((6, 2048, 128), F), pltpu.VMEM((1536, 768), B),
            pltpu.VMEM((1536, 768), B), pltpu.VMEM((6, 1440, 128), F), pltpu.VMEM((6, 1440, 128), F)]


def prepare(at, *args):
    return pl.pallas_call(
        prepare_kernel, out_shape=(shape_of(16, 216), shape_of(48, 128), shape_of(24, 216)),
        in_specs=[SM] + [HB] * 9, out_specs=(VM,) * 3,
        scratch_shapes=[pltpu.VMEM(x.shape, B) for x in args] + [pltpu.SemaphoreType.DMA((9,))],
        name="prepare")(at, *args)


def pieces(turned, piece):
    return pl.pallas_call(pieces_kernel, out_shape=(shape_of(24, 216), shape_of(16, 128), shape_of(8, 240)),
                          in_specs=[VM, VM], out_specs=(VM,) * 3, name="pieces",
                          compiler_params=params(4))(turned, piece)


def form_copies():
    return [pltpu.VMEM((1296, 1408), B), pltpu.VMEM((1296, 1536), B), pltpu.SemaphoreType.DMA((2,))]


def upper(order, bufs, small, wtop, wright):
    return pl.pallas_call(
        upper_kernel, out_shape=(shape_of(216, 216), shape_of(6, 216)), in_specs=[SM] + [VM] * 9 + [HB] * 2,
        out_specs=(VM, VM), scratch_shapes=scratch() + [pltpu.VMEM((320, 128), F)] + form_copies(), name="upper",
        compiler_params=params(50), cost_estimate=work(8 << 30))(order, *bufs, small, wtop, wright)


def left(order, bufs, small, ber, wtop, wbot, bpr):
    return pl.pallas_call(
        left_kernel, out_shape=(shape_of(216, 216), shape_of(128, 256, kind=F)),
        in_specs=[SM] + [VM] * 10 + [HB] * 2 + [VM], out_specs=(VM, VM),
        scratch_shapes=scratch() + [pltpu.VMEM((288, 128), F)] + form_copies(), name="left",
        compiler_params=params(50), cost_estimate=work(8 << 30))(order, *bufs, small, ber, wtop, wbot, bpr)


def finish_kernel(own, one, two, three, out_ref):
    res = own[...] + one[...] + two[...] + three[...]
    rows = [jnp.concatenate([res[a:a + 1, x * 36:(x + 1) * 36] for a in range(6)], axis=1) for x in range(6)]
    out_ref[...] = jnp.concatenate(rows, axis=0).astype(B)


def finish(*parts):
    return pl.pallas_call(finish_kernel, out_shape=shape_of(6, 216), in_specs=[VM] * 4, out_specs=VM,
                          name="finish", compiler_params=params(4))(*parts)


def lane_pattern(ref):
    k = lax.broadcasted_iota(jnp.int32, (256, 256), 0)
    n = lax.broadcasted_iota(jnp.int32, (256, 256), 1)
    w = n % 128
    ref[...] = jnp.where(w < 108, k - (n // 128) * 36 - w % 36, -1)


def lanes_shifted(a_ref, z_ref, pattern, pair):
    tile = (pair * 72) // 128
    base = pl.multiple_of(tile * 128, 128)
    off = pair * 72 - tile * 128
    sel = (pattern[...] == off).astype(B)
    z_ref[...] = dot(a_ref[:, pl.ds(base, 256)], sel)


def column_chunks(src, dst, sems):
    ends = (0, 384, 768, 1152, 1408)
    return load([(src.at[:, p:q], dst.at[:, p:q]) for p, q in zip(ends, ends[1:])], sems)


def realign(a_ref, z_ref, o_ref, pattern, out_hbm, sem, chunks=()):
    lane = lax.broadcasted_iota(jnp.int32, (36, 128), 1)

    def f(g, _):
        for n, cp in zip((0, 2, 4, 7), chunks):
            @pl.when(g == n)
            def _(cp=cp):
                cp.wait()
        strips = []
        for h in range(2):
            lanes_shifted(a_ref, z_ref.at[h], pattern, 2 * g + h)
        for h in range(2):
            for q in range(2):
                tiles = []
                for m in range(12):
                    z = [z_ref[h, (3 * m + e) * 36:(3 * m + e + 1) * 36, q * 128:(q + 1) * 128] for e in range(3)]
                    tiles.append(jnp.where(lane < 36, z[0], jnp.where(lane < 72, z[1], z[2])))
                strips.append(jnp.concatenate(tiles, axis=1))
        at = pl.multiple_of(g * 144, 16)
        o_ref[pl.ds(at, 144), :] = jnp.concatenate(strips, axis=0).astype(B)
        pltpu.make_async_copy(o_ref.at[pl.ds(at, 144), :], out_hbm.at[pl.ds(at, 144), :], sem.at[g]).start()
        return 0
    lax.fori_loop(0, 9, f, 0)

    def w(g, _):
        at = pl.multiple_of(g * 144, 16)
        pltpu.make_async_copy(o_ref.at[pl.ds(at, 144), :], out_hbm.at[pl.ds(at, 144), :], sem.at[g]).wait()
        return 0
    lax.fori_loop(0, 9, w, 0)


def right_form_kernel(s_hbm, wright_hbm, apad, z, o, pattern, sems, done):
    chunks = column_chunks(s_hbm, apad, sems)
    lane_pattern(pattern)
    realign(apad, z, o, pattern, wright_hbm, done, chunks)


def left_forms_kernel(s_hbm, wtop_hbm, wbot_hbm, apad, z, o, pattern, sems, done, s_ref):
    chunks = column_chunks(s_hbm, s_ref, sems)
    lane_pattern(pattern)
    eye = (lax.broadcasted_iota(jnp.int32, (128, 128), 0) == lax.broadcasted_iota(jnp.int32, (128, 128), 1)).astype(B)
    for b in range(11):
        n = min(128, 1296 - b * 128)
        if b % 3 == 0:
            chunks[b // 3].wait()
        apad[b * 128:b * 128 + n, :1296] = dot(eye[:n, :n], s_ref[:, b * 128:b * 128 + n], NT).astype(B)
    apad[:, 1296:1408] = jnp.zeros((1296, 112), B)
    out = pltpu.make_async_copy(apad, wtop_hbm, sems.at[0])
    out.start()
    realign(apad, z, o, pattern, wbot_hbm, done)
    out.wait()


def flat_form_kernel(x_ref, s_hbm, wide, tiles, s_ref, sems):
    def widen(i, _):
        at = pl.multiple_of(i * 256, 16)
        wide[pl.ds(at, 256), :] = x_ref[pl.ds(at, 256), :].astype(F)
        return 0
    lax.fori_loop(0, 51, widen, 0)
    wide[13056:13122, :] = x_ref[13056:13122, :].astype(F)
    lane = lax.broadcasted_iota(jnp.int32, (162, 128), 1)
    for i in range(8):
        def turn(j):
            v = wide[pl.ds(10 * i + j, 162, stride=81), :]
            return pltpu.roll(v, 128 - 16 * i, 1) if i else v
        here = turn(0)
        for j in range(11):
            if j == 10:
                tile = jnp.where(lane < 16, here, 0.0)
            else:
                after = turn(j + 1)
                tile = jnp.where(lane < 128 - 16 * i, here, after) if i else here
                here = after
            tiles[j, pl.ds(i, 162, stride=8), :] = tile

    def narrow(g, _):
        at = pl.multiple_of(g * 144, 16)
        for j in range(11):
            s_ref[pl.ds(at, 144), 128 * j:128 * j + 128] = tiles[j, pl.ds(at, 144), :].astype(B)
        pltpu.make_async_copy(s_ref.at[pl.ds(at, 144), :], s_hbm.at[pl.ds(at, 144), :], sems.at[g]).start()
        return 0
    lax.fori_loop(0, 9, narrow, 0)

    def w(g, _):
        at = pl.multiple_of(g * 144, 16)
        pltpu.make_async_copy(s_ref.at[pl.ds(at, 144), :], s_hbm.at[pl.ds(at, 144), :], sems.at[g]).wait()
        return 0
    lax.fori_loop(0, 9, w, 0)


def form_scratch():
    return [pltpu.VMEM((1296, 1408), B), pltpu.VMEM((2, 1296, 256), F), pltpu.VMEM((1296, 1536), B),
            pltpu.VMEM((256, 256), jnp.int32),
            pltpu.SemaphoreType.DMA((4,)), pltpu.SemaphoreType.DMA((9,))]


def flat_form(flat):
    return pl.pallas_call(flat_form_kernel, out_shape=shape_of(1296, 1408), in_specs=[VM], out_specs=HB,
                          scratch_shapes=[pltpu.VMEM((13616, 128), F), pltpu.VMEM((11, 1344, 128), F),
                                          pltpu.VMEM((1296, 1408), B), pltpu.SemaphoreType.DMA((9,))],
                          name="flat_form", compiler_params=params(60), cost_estimate=work(3 << 30))(flat)


def right_form(s2):
    return pl.pallas_call(right_form_kernel, out_shape=shape_of(1296, 1536), in_specs=[HB], out_specs=HB,
                          scratch_shapes=form_scratch(), name="right_form", compiler_params=params(60),
                          cost_estimate=work(3 << 30))(s2)


def left_forms(s2):
    return pl.pallas_call(left_forms_kernel, out_shape=(shape_of(1296, 1408), shape_of(1296, 1536)), in_specs=[HB],
                          out_specs=(HB, HB), scratch_shapes=form_scratch() + [pltpu.VMEM((1296, 1408), B)],
                          name="left_forms", compiler_params=params(60), cost_estimate=work(4 << 30))(s2)


ROW, COL = "row", "col"


def row_permute(x, move):
    pairs = []
    for y in range(4):
        for z in range(2):
            for k in range(2):
                a, b, c = move(y, z, k)
                pairs.append((y * 4 + z * 2 + k, a * 4 + b * 2 + c))
    return lax.ppermute(x, ROW, pairs)


def col_permute(x, move):
    pairs = []
    for z in range(4):
        for i in range(4):
            a, b = move(z, i)
            pairs.append((z * 4 + i, a * 4 + b))
    return lax.ppermute(x, COL, pairs)


def swap_axes(x):
    pairs = [(r * 16 + c, c * 16 + r) for r in range(16) for c in range(16)]
    return lax.ppermute(x, (ROW, COL), pairs)


def stacked(own, received):
    return jnp.concatenate([own, *received], axis=0)


def other_core(x):
    return row_permute(x, lambda a, b, k: (a, b, 1 - k))


def other_z(x):
    return row_permute(x, lambda a, b, k: (a, 1 - b, k))


def along_y(x, s):
    return row_permute(x, lambda a, b, k: ((a + s) % 4, b, k))


def shards(uc, rc, lc, te, re, be, le, site_flat, tp, bp):
    r = lax.axis_index(ROW)
    c = lax.axis_index(COL)
    y, zlo, core = r // 4, (r // 2) % 2, r % 2
    zhi, x = c // 4, c % 4
    hold = lax.optimization_barrier

    piece, pack, turned = prepare((r * 6).astype(jnp.int32).reshape(1), te, re, be, le, uc.T, rc.T, lc.T, tp.T, bp.T)
    swapped = swap_axes(turned)
    s2 = flat_form(hold((site_flat, turned))[0].reshape(13122, 128))
    swapped, s2 = hold((swapped, s2))
    piece, tpx, bpr = pieces(swapped, piece)

    piece = stacked(piece, [col_permute(piece, lambda z, i, s=s: ((z + s) % 4, i)) for s in (1, 2, 3)])
    piece = stacked(piece, [col_permute(piece, lambda z, i, s=s: (z, (i + s) % 4)) for s in (1, 2, 3)])
    at = jnp.arange(384)
    x_rel, z_rel, edge, j = at // 96, (at // 24) % 4, (at // 8) % 3, at % 8
    block = ((zhi - z_rel) % 4) * 4 + (x - x_rel) % 4
    target = jnp.where(j < 6, edge * 128 + block * 6 + j, -1)
    place = (target[:, None] == at[None, :]).astype(B)
    rows = lax.dot_general(piece, place, (((0,), (0,)), ((), ())), preferred_element_type=F).astype(B)
    ber = rows[:, 256:]

    own = jnp.concatenate([rows[:, :128], rows[:, 128:256], pack, tpx], axis=0)
    beside = other_z(own)
    wright = right_form(hold((s2, own))[0])
    beside, wright = hold((beside, wright))
    near = stacked(own, [beside])
    far = [along_y(near, s) for s in (1, 2, 3)]
    near_twin = other_core(near)
    wtop, wbot = left_forms(hold((s2, near))[0])
    *far, near_twin, wtop = hold((*far, near_twin, wtop))
    far_twin = [other_core(f) for f in far]
    bufs = [near, *far, near_twin, *far_twin]
    rel = jnp.arange(16)
    order = ((y - (rel // 2) % 4) % 4) * 4 + (zlo ^ (rel % 2)) * 2 + (core ^ (rel // 8))
    order = order.astype(jnp.int32)

    small = gather_small(order, bufs)

    lf, cb = left(order, bufs, small, ber, wtop, wbot, bpr)
    part = lambda v, n, size: lax.dynamic_slice_in_dim(v, n * size, size, 0)
    mine = lambda k, z: part(cb, k * 2 + z, 32)
    near_sums = [other_core(mine(1 - core, zlo)), other_z(mine(core, 1 - zlo)),
                 row_permute(mine(1 - core, 1 - zlo), lambda a, b, k: (a, 1 - b, 1 - k))]
    cb = mine(core, zlo) + near_sums[0] + near_sums[1] + near_sums[2]
    cb_y = [along_y(part(cb, (y + s) % 4, 8), s) for s in (1, 2, 3)]
    order = hold((order, cb))[0]
    up, corner_top = upper(order, bufs, small, wtop, wright)
    *cb_y, up = hold((*cb_y, up))
    corner_bottom = finish(part(cb, y, 8), *cb_y)
    return up, lf, corner_top, corner_bottom


def solution(mesh):
    placed = (
        P(None, ROW),
        P(None, ROW),
        P(None, ROW),
        P(ROW, COL, None),
        P(ROW, COL, None),
        P(ROW, COL, None),
        P(ROW, COL, None),
        P(),
        P(COL, None),
        P(COL, None),
    )
    return jax.shard_map(
        shards,
        mesh=mesh,
        in_specs=placed,
        out_specs=(P(ROW, COL), P(COL, ROW), P(COL, ROW), P(COL, ROW)),
        check_vma=False,
    )
```
